128 devices in a mesh: row: 16 (over z_hi, x, core), col: 8 (over y, z_lo).
Axes of the slice: x: 4, y: 4, z: 4 (z_hi: 2, z_lo: 2; z = z_hi * 2 + z_lo), core: 2. Of those that a mesh axis runs over, the one named last changes fastest.
Arguments:
- pair: bfloat16 [512, 512, 128], P('row', 'col'), may hold values from -6 to 6
- cotangent: bfloat16 [512, 512, 128], P('row', 'col'), may hold values from -6 to 6
- length: int32 [1], replicated, may hold values from 256 to 512
- norm_gain: float32 [128], replicated, may hold values from 0.1 to 1.9
- norm_bias: float32 [128], replicated, may hold values from -1.5 to 1.5
- left_weight: bfloat16 [128, 256], replicated, may hold values from -0.5 to 0.5
- right_weight: bfloat16 [128, 256], replicated, may hold values from -0.5 to 0.5
- gate_weight: bfloat16 [128, 128], replicated, may hold values from -0.5 to 0.5
- out_gain: float32 [128], replicated, may hold values from 0.1 to 1.9
- out_bias: float32 [128], replicated, may hold values from -2 to 2
- out_weight: bfloat16 [128, 128], replicated, may hold values from -0.5 to 0.5
Outputs:
- update: bfloat16 [512, 512, 128], P('row', 'col')
- grad_pair: bfloat16 [512, 512, 128], P('row', 'col')
- grad_left: float32 [128, 256], replicated
- grad_right: float32 [128, 256], replicated
- grad_gating: float32 [128, 128], replicated
- grad_output: float32 [128, 128], replicated
- grad_norms: float32 [4, 128], replicated
The draws below stay inside these ranges and needn't reach their ends.
Inputs may be any that keep to these rules, and one draw needn't show every extreme that they name: Tokens at positions 511 down to length are padding.
All inputs are finite; a program needn't handle non-finite values.
Results may differ from the reference program's by a relative error of at most 0.014.
Values may be sent and summed in bfloat16 or wider, within the bound.
A program may use at most 128 MiB of HBM per device.

```python
import jax
import jax.numpy as jnp
from jax import lax

PAIR = 128
HIDDEN_SIZE = 128
ROW_DEV = 32
TOKENS = 512
COL_DEV = 64
N_ROW = 16
N_COL = 8


def shard_levels(rng, shape, split, smallest, high):
    level, own = 1.0, jax.random.fold_in(rng, 6)
    for position, parts in split:
        draws = jnp.exp(jax.random.uniform(jax.random.fold_in(own, position), (parts,), jnp.float32, smallest / len(split), high / len(split)))
        level = level * jnp.repeat(draws, shape[position] // parts).reshape([-1 if axis == position else 1 for axis in range(len(shape))])
    return level


def normal_values(rng, dims, scale, bound, split=(), kind=jnp.bfloat16):
    entries = jax.random.normal(rng, dims, jnp.float32) * scale
    if len(split) > 0:
        entries = shard_levels(rng, dims, split, -0.22, 0.18) * entries
    return jnp.clip(entries, min=-bound, max=bound).astype(kind)


def setup_inputs(seed: int = 0) -> dict:
    key_list = jax.random.split(jax.random.key(seed), 12)
    pair = normal_values(key_list[0], (TOKENS, TOKENS, PAIR), 1.0, 6.0, ((0, 16), (1, 8)))
    cotangent = normal_values(key_list[1], (TOKENS, TOKENS, PAIR), 1.0, 6.0, ((0, 16), (1, 8)))
    length = jax.random.randint(key_list[2], (1,), TOKENS // 2, TOKENS + 1).astype(jnp.int32)
    norm_gain = jnp.clip(1.0 + 0.18 * jax.random.normal(key_list[3], (PAIR,), jnp.float32), 0.1, 1.9)
    norm_bias = normal_values(key_list[4], (PAIR,), 0.3, 1.5, (), jnp.float32)
    left_weight = normal_values(key_list[5], (PAIR, 2 * HIDDEN_SIZE), PAIR ** -0.5, 0.5)
    right_weight = normal_values(key_list[6], (PAIR, 2 * HIDDEN_SIZE), PAIR ** -0.5, 0.5)
    gate_weight = normal_values(key_list[7], (PAIR, PAIR), PAIR ** -0.5, 0.5)
    out_gain = jnp.clip(1.0 + 0.18 * jax.random.normal(key_list[8], (HIDDEN_SIZE,), jnp.float32), 0.1, 1.9)
    out_bias = normal_values(key_list[9], (HIDDEN_SIZE,), 0.5, 2.0, (), jnp.float32)
    out_weight = normal_values(key_list[10], (HIDDEN_SIZE, PAIR), HIDDEN_SIZE ** -0.5, 0.5)
    return dict(pair=pair, cotangent=cotangent, length=length, norm_gain=norm_gain, norm_bias=norm_bias, left_weight=left_weight, right_weight=right_weight, gate_weight=gate_weight, out_gain=out_gain, out_bias=out_bias, out_weight=out_weight)


EPS = 1e-05

def normalize(values):
    center = values - lax.optimization_barrier(jnp.mean(values, axis=-1, keepdims=True))
    inverse = lax.rsqrt(lax.optimization_barrier(jnp.mean(center * center, axis=-1, keepdims=True)) + EPS)
    return (center * inverse, inverse)

def product(form, first, second):
    return jnp.einsum(form, first.astype(jnp.float32), second.astype(jnp.float32), precision=lax.Precision.HIGHEST)

def rounded(values):
    return lax.optimization_barrier(values.astype(jnp.bfloat16)).astype(jnp.float32)

def reference(pair, cotangent, length, norm_gain, norm_bias, left_weight, right_weight, gate_weight, out_gain, out_bias, out_weight):
    pair_hat, pair_scale = normalize(pair.astype(jnp.float32))
    normed = (pair_hat * norm_gain + norm_bias).astype(jnp.bfloat16)
    valid = (jnp.arange(TOKENS, dtype=jnp.int32) < length[0]).astype(jnp.float32)
    pad_mask = (valid[:, None] * valid[None, :])[..., None]

    def gating(weight):
        projected = product('ikc,ch->ikh', normed, weight)
        values = projected[..., :HIDDEN_SIZE]
        sigmoid_val = jax.nn.sigmoid(projected[..., HIDDEN_SIZE:])
        return ((pad_mask * sigmoid_val * values).astype(jnp.bfloat16), values, sigmoid_val)
    left_act, left_val, left_sig = gating(left_weight)
    right_act, right_val, right_sig = gating(right_weight)
    tri = product('ikh,jkh->ijh', left_act, right_act)
    tri_hat, tri_scale = normalize(tri)
    tri_normed = (tri_hat * out_gain + out_bias).astype(jnp.bfloat16)
    outer_val = product('ijh,hc->ijc', tri_normed, out_weight)
    gate_val = jax.nn.sigmoid(product('ijc,cd->ijd', normed, gate_weight))
    update = (gate_val * outer_val).astype(jnp.bfloat16)
    upstream = cotangent.astype(jnp.float32)
    outer_grad = (upstream * gate_val).astype(jnp.bfloat16)
    gate_grad = (upstream * outer_val * gate_val * (1.0 - gate_val)).astype(jnp.bfloat16)
    grad_output = product('ijh,ijc->hc', tri_normed, outer_grad)
    grad_gating = product('ijc,ijd->cd', normed, gate_grad)
    tnorm_grad = product('ijc,hc->ijh', outer_grad, out_weight)
    hat_grad = tnorm_grad * out_gain
    tri_grad = (tri_scale * (hat_grad - lax.optimization_barrier(jnp.mean(hat_grad, axis=-1, keepdims=True)) - tri_hat * lax.optimization_barrier(jnp.mean(hat_grad * tri_hat, axis=-1, keepdims=True)))).astype(jnp.bfloat16)
    row_part = jnp.zeros((TOKENS, TOKENS, HIDDEN_SIZE), jnp.float32)
    for column in range(N_COL):
        lower = column * COL_DEV
        row_part = row_part + rounded(product('ijh,jkh->ikh', tri_grad[:, lower:lower + COL_DEV], right_act[lower:lower + COL_DEV]))
    col_part = jnp.zeros((TOKENS, TOKENS, HIDDEN_SIZE), jnp.float32)
    for row_block in range(N_ROW):
        lower = row_block * ROW_DEV
        col_part = col_part + rounded(product('ijh,ikh->jkh', tri_grad[lower:lower + ROW_DEV], left_act[lower:lower + ROW_DEV]))
    col_part = rounded(col_part)

    def push_back(partial_value, values, sigmoid_val, weight):
        combined = jnp.concatenate([partial_value * pad_mask * sigmoid_val, partial_value * pad_mask * values * sigmoid_val * (1.0 - sigmoid_val)], axis=-1).astype(jnp.bfloat16)
        return (product('ikh,ch->ikc', combined, weight), product('ikc,ikh->ch', normed, combined))
    from_rows, grad_left = push_back(row_part, left_val, left_sig, left_weight)
    from_cols, grad_right = push_back(col_part, right_val, right_sig, right_weight)
    normed_grad = product('ijd,cd->ijc', gate_grad, gate_weight) + from_rows + from_cols
    scaled = normed_grad * norm_gain
    grad_pair = (pair_scale * (scaled - lax.optimization_barrier(jnp.mean(scaled, axis=-1, keepdims=True)) - pair_hat * lax.optimization_barrier(jnp.mean(scaled * pair_hat, axis=-1, keepdims=True)))).astype(jnp.bfloat16)
    grad_norms = jnp.stack([lax.optimization_barrier(jnp.sum(normed_grad * pair_hat, axis=(0, 1))), lax.optimization_barrier(jnp.sum(normed_grad, axis=(0, 1))), lax.optimization_barrier(jnp.sum(tnorm_grad * tri_hat, axis=(0, 1))), lax.optimization_barrier(jnp.sum(tnorm_grad, axis=(0, 1)))])
    inverse = 1.0 / TOKENS
    return (update, grad_pair, grad_left * inverse, grad_right * inverse, grad_gating * inverse, grad_output * inverse, grad_norms * inverse)
```

```python
import jax
import jax.numpy as jnp
from jax import lax
from jax.sharding import PartitionSpec as P

EPS = 1e-05
AXES = ("row", "col")


def normalize(values):
    center = values - jnp.mean(values, axis=-1, keepdims=True)
    inverse = lax.rsqrt(jnp.mean(center * center, axis=-1, keepdims=True) + EPS)
    return (center * inverse, inverse)


def exchange(x):
    return lax.all_to_all(x, AXES, 0, 0, tiled=True)


def per_device(
    pair,
    cotangent,
    length,
    norm_gain,
    norm_bias,
    left_weight,
    right_weight,
    gate_weight,
    out_gain,
    out_bias,
    out_weight,
):
    n_row = lax.axis_size("row")
    n_col = lax.axis_size("col")
    n = n_row * n_col
    rows, cols = pair.shape[:2]
    tokens = rows * n_row
    hidden = out_weight.shape[0]
    row_at = lax.axis_index("row") * rows
    col_at = lax.axis_index("col") * cols
    first_ok = row_at + jnp.arange(rows, dtype=jnp.int32) < length[0]
    second_ok = col_at + jnp.arange(cols, dtype=jnp.int32) < length[0]
    mask = (first_ok[:, None] & second_ok[None, :]).astype(jnp.float32).reshape(1, -1)

    def to_owner(tiles):
        return exchange(jnp.stack([t.reshape(n, rows * cols // 128, 128) for t in tiles], axis=1))

    def whole(received):
        return received.reshape(n_row, n_col, rows, cols).transpose(0, 2, 1, 3).reshape(tokens, tokens)

    def tiled(matrix):
        t = matrix.reshape(n_row, rows, n_col, cols).transpose(0, 2, 1, 3)
        return t.reshape(n, rows * cols // 128, 128)

    pair_hat, pair_scale = normalize(pair.astype(jnp.float32))
    normed = (pair_hat * norm_gain + norm_bias).astype(jnp.bfloat16)
    flat = normed.reshape(rows * cols, -1)

    def dot(form, a, b):
        return jnp.einsum(form, a, b, preferred_element_type=jnp.float32)

    def gating(weight):
        projected = dot("pc,ch->hp", flat, weight)
        values = projected[:hidden]
        sig = jax.nn.sigmoid(projected[hidden:])
        return (mask * sig * values).astype(jnp.bfloat16), values, sig

    left, left_val, left_sig = gating(left_weight)
    right, right_val, right_sig = gating(right_weight)
    got = to_owner([left, right])
    big_l = whole(got[:, 0])
    big_r = whole(got[:, 1])
    tri_own = dot("ik,jk->ij", big_l, big_r).astype(jnp.bfloat16)
    tri = exchange(tiled(tri_own)).reshape(hidden, -1).astype(jnp.float32)
    center = tri - jnp.mean(tri, axis=0, keepdims=True)
    tri_scale = lax.rsqrt(jnp.mean(center * center, axis=0, keepdims=True) + EPS)
    tri_hat = center * tri_scale
    tri_normed = (tri_hat * out_gain[:, None] + out_bias[:, None]).astype(jnp.bfloat16)
    outer = dot("hp,hc->cp", tri_normed, out_weight)
    gate = jax.nn.sigmoid(dot("pc,cd->dp", flat, gate_weight))
    update = (gate * outer).astype(jnp.bfloat16).T.reshape(pair.shape)
    upstream = cotangent.reshape(rows * cols, -1).T.astype(jnp.float32)
    outer_grad = (upstream * gate).astype(jnp.bfloat16)
    gate_grad = (upstream * outer * gate * (1.0 - gate)).astype(jnp.bfloat16)
    grad_output = dot("hp,cp->hc", tri_normed, outer_grad)
    grad_gating = dot("pc,dp->cd", flat, gate_grad)
    tnorm_grad = dot("cp,hc->hp", outer_grad, out_weight)
    hat_grad = tnorm_grad * out_gain[:, None]
    tri_grad = (
        tri_scale
        * (
            hat_grad
            - jnp.mean(hat_grad, axis=0, keepdims=True)
            - tri_hat * jnp.mean(hat_grad * tri_hat, axis=0, keepdims=True)
        )
    ).astype(jnp.bfloat16)
    g = whole(exchange(tri_grad.reshape(n, rows * cols // 128, 128)))
    row_own = dot("ij,jk->ik", g, big_r).astype(jnp.bfloat16)
    col_own = dot("ij,ik->jk", g, big_l).astype(jnp.bfloat16)
    back = exchange(jnp.stack([tiled(row_own), tiled(col_own)], axis=1))
    row_part = back[:, 0].reshape(hidden, -1).astype(jnp.float32)
    col_part = back[:, 1].reshape(hidden, -1).astype(jnp.float32)

    def push_back(part, values, sig, weight):
        comb = jnp.concatenate(
            [part * mask * sig, part * mask * values * sig * (1.0 - sig)], axis=0
        ).astype(jnp.bfloat16)
        return dot("hp,ch->pc", comb, weight), dot("pc,hp->ch", flat, comb)

    from_rows, grad_left = push_back(row_part, left_val, left_sig, left_weight)
    from_cols, grad_right = push_back(col_part, right_val, right_sig, right_weight)
    gate_back = dot("dp,cd->pc", gate_grad, gate_weight)
    normed_grad = (gate_back + from_rows + from_cols).reshape(pair.shape)
    scaled = normed_grad * norm_gain
    grad_pair = (
        pair_scale
        * (
            scaled
            - jnp.mean(scaled, axis=-1, keepdims=True)
            - pair_hat * jnp.mean(scaled * pair_hat, axis=-1, keepdims=True)
        )
    ).astype(jnp.bfloat16)
    grad_norms = jnp.stack(
        [
            jnp.sum(normed_grad * pair_hat, axis=(0, 1)),
            jnp.sum(normed_grad, axis=(0, 1)),
            jnp.sum(tnorm_grad * tri_hat, axis=1),
            jnp.sum(tnorm_grad, axis=1),
        ]
    )
    parts = [grad_left, grad_right, grad_gating, grad_output, grad_norms]
    flat_parts = jnp.concatenate([a.reshape(-1, 128) for a in parts], axis=0)
    size = flat_parts.shape[0]
    per = -(-size // (n * 8)) * 8
    padded = jnp.pad(flat_parts, ((0, per * n - size), (0, 0))).reshape(n, per, 128)
    mine = jnp.sum(exchange(padded), axis=0) * (1.0 / tokens)
    total = lax.all_gather(mine, AXES, axis=0, tiled=True)
    done, at = [], 0
    for a in parts:
        count = a.size // 128
        done.append(total[at : at + count].reshape(a.shape))
        at += count
    return (update, grad_pair, *done)


def solution(mesh):
    return jax.shard_map(
        per_device,
        mesh=mesh,
        in_specs=(P("row", "col", None), P("row", "col", None)) + (P(),) * 9,
        out_specs=(P("row", "col", None), P("row", "col", None)) + (P(),) * 5,
        check_vma=False,
    )
```

```python
import jax
import jax.numpy as jnp
from jax import lax
from jax.sharding import PartitionSpec as P

EPS = 1e-05
AXES = ("row", "col")


def normalize(values):
    center = values - jnp.mean(values, axis=-1, keepdims=True)
    inverse = lax.rsqrt(jnp.mean(center * center, axis=-1, keepdims=True) + EPS)
    return (center * inverse, inverse)


def exchange(x):
    return lax.all_to_all(x, AXES, 0, 0, tiled=True)


def per_device(
    pair,
    cotangent,
    length,
    norm_gain,
    norm_bias,
    left_weight,
    right_weight,
    gate_weight,
    out_gain,
    out_bias,
    out_weight,
):
    n_row = lax.axis_size("row")
    n_col = lax.axis_size("col")
    n = n_row * n_col
    rows, cols = pair.shape[:2]
    tokens = rows * n_row
    hidden = out_weight.shape[0]
    row_at = lax.axis_index("row") * rows
    col_at = lax.axis_index("col") * cols
    first_ok = row_at + jnp.arange(rows, dtype=jnp.int32) < length[0]
    second_ok = col_at + jnp.arange(cols, dtype=jnp.int32) < length[0]
    mask = (first_ok[:, None] & second_ok[None, :]).astype(jnp.float32).reshape(1, -1)

    def to_owner(tiles):
        return exchange(jnp.stack([t.reshape(n, rows * cols // 128, 128) for t in tiles], axis=1))

    def whole(received):
        return received.reshape(n_row, n_col, rows, cols).transpose(0, 2, 1, 3).reshape(tokens, tokens)

    def tiled(matrix):
        t = matrix.reshape(n_row, rows, n_col, cols).transpose(0, 2, 1, 3)
        return t.reshape(n, rows * cols // 128, 128)

    pair_hat, pair_scale = normalize(pair.astype(jnp.float32))
    normed = (pair_hat * norm_gain + norm_bias).astype(jnp.bfloat16)
    flat = normed.reshape(rows * cols, -1)

    def dot(form, a, b):
        return jnp.einsum(form, a, b, preferred_element_type=jnp.float32)

    def gating(weight):
        projected = dot("pc,ch->hp", flat, weight)
        values = projected[:hidden]
        sig = jax.nn.sigmoid(projected[hidden:])
        return (mask * sig * values).astype(jnp.bfloat16), values, sig

    left, left_val, left_sig = gating(left_weight)
    right, right_val, right_sig = gating(right_weight)
    got = to_owner([left, right])
    big_l = whole(got[:, 0])
    big_r = whole(got[:, 1])
    tri_own = dot("ik,jk->ij", big_l, big_r).astype(jnp.bfloat16)
    tri = exchange(tiled(tri_own)).reshape(hidden, -1).astype(jnp.float32)
    center = tri - jnp.mean(tri, axis=0, keepdims=True)
    tri_scale = lax.rsqrt(jnp.mean(center * center, axis=0, keepdims=True) + EPS)
    tri_hat = center * tri_scale
    tri_normed = (tri_hat * out_gain[:, None] + out_bias[:, None]).astype(jnp.bfloat16)
    outer = dot("hp,hc->cp", tri_normed, out_weight)
    gate = jax.nn.sigmoid(dot("pc,cd->dp", flat, gate_weight))
    update = (gate * outer).astype(jnp.bfloat16).T.reshape(pair.shape)
    upstream = cotangent.reshape(rows * cols, -1).T.astype(jnp.float32)
    outer_grad = (upstream * gate).astype(jnp.bfloat16)
    gate_grad = (upstream * outer * gate * (1.0 - gate)).astype(jnp.bfloat16)
    grad_output = dot("hp,cp->hc", tri_normed, outer_grad)
    grad_gating = dot("pc,dp->cd", flat, gate_grad)
    tnorm_grad = dot("cp,hc->hp", outer_grad, out_weight)
    hat_grad = tnorm_grad * out_gain[:, None]
    tri_grad = (
        tri_scale
        * (
            hat_grad
            - jnp.mean(hat_grad, axis=0, keepdims=True)
            - tri_hat * jnp.mean(hat_grad * tri_hat, axis=0, keepdims=True)
        )
    ).astype(jnp.bfloat16)
    g = whole(exchange(tri_grad.reshape(n, rows * cols // 128, 128)))
    row_own = dot("ij,jk->ik", g, big_r).astype(jnp.bfloat16)
    col_own = dot("ij,ik->jk", g, big_l).astype(jnp.bfloat16)
    back = exchange(jnp.stack([tiled(row_own), tiled(col_own)], axis=1))
    row_part = back[:, 0].reshape(hidden, -1).astype(jnp.float32)
    col_part = back[:, 1].reshape(hidden, -1).astype(jnp.float32)

    def push_back(part, values, sig, weight):
        comb = jnp.concatenate(
            [part * mask * sig, part * mask * values * sig * (1.0 - sig)], axis=0
        ).astype(jnp.bfloat16)
        return dot("hp,ch->pc", comb, weight), dot("pc,hp->ch", flat, comb)

    from_rows, grad_left = push_back(row_part, left_val, left_sig, left_weight)
    from_cols, grad_right = push_back(col_part, right_val, right_sig, right_weight)
    gate_back = dot("dp,cd->pc", gate_grad, gate_weight)
    normed_grad = (gate_back + from_rows + from_cols).reshape(pair.shape)
    scaled = normed_grad * norm_gain
    grad_pair = (
        pair_scale
        * (
            scaled
            - jnp.mean(scaled, axis=-1, keepdims=True)
            - pair_hat * jnp.mean(scaled * pair_hat, axis=-1, keepdims=True)
        )
    ).astype(jnp.bfloat16)
    grad_norms = jnp.stack(
        [
            jnp.sum(normed_grad * pair_hat, axis=(0, 1)),
            jnp.sum(normed_grad, axis=(0, 1)),
            jnp.sum(tnorm_grad * tri_hat, axis=1),
            jnp.sum(tnorm_grad, axis=1),
        ]
    )
    parts = [grad_left, grad_right, grad_gating, grad_output, grad_norms]
    flat_parts = jnp.concatenate([a.reshape(-1, 128) for a in parts], axis=0)
    size = flat_parts.shape[0]
    per = -(-size // (n * 8)) * 8
    padded = jnp.pad(flat_parts, ((0, per * n - size), (0, 0))).reshape(n, per, 128)
    mine = jnp.sum(exchange(padded), axis=0) * (1.0 / tokens)
    total = exchange(jnp.broadcast_to(mine[None], (n,) + mine.shape)).reshape(n * per, 128)
    done, at = [], 0
    for a in parts:
        count = a.size // 128
        done.append(total[at : at + count].reshape(a.shape))
        at += count
    return (update, grad_pair, *done)


def solution(mesh):
    return jax.shard_map(
        per_device,
        mesh=mesh,
        in_specs=(P("row", "col", None), P("row", "col", None)) + (P(),) * 9,
        out_specs=(P("row", "col", None), P("row", "col", None)) + (P(),) * 5,
        check_vma=False,
    )
```

```python
import functools

import jax
import jax.numpy as jnp
from jax import lax
from jax.experimental import pallas as pl
from jax.experimental.pallas import tpu as pltpu
from jax.sharding import PartitionSpec as P

EPS = 1e-05
AXES = ("row", "col")


def normalize(values):
    center = values - jnp.mean(values, axis=-1, keepdims=True)
    inverse = lax.rsqrt(jnp.mean(center * center, axis=-1, keepdims=True) + EPS)
    return (center * inverse, inverse)


MESH = pl.DeviceIdType.MESH


def exchange_kernel(n_row, n_col, src, dst, send_sem, recv_sem):
    n = n_row * n_col
    me = lax.axis_index("row") * n_col + lax.axis_index("col")

    def coords(p):
        return (p // n_col, lax.rem(p, n_col))

    def greet(d, carry):
        peer = lax.rem(me + d, n)
        pl.semaphore_signal(barrier, inc=1, device_id=coords(peer), device_id_type=MESH)
        return carry

    def send(d, carry):
        peer = lax.rem(me + d, n)
        pltpu.make_async_remote_copy(
            src_ref=src.at[peer],
            dst_ref=dst.at[me],
            send_sem=send_sem,
            recv_sem=recv_sem,
            device_id=coords(peer),
            device_id_type=MESH,
        ).start()
        return carry

    barrier = pltpu.get_barrier_semaphore()
    lax.fori_loop(1, n, greet, 0)
    pl.semaphore_wait(barrier, n - 1)
    lax.fori_loop(1, n, send, 0)
    dst[me] = src[me]
    others = dst.at[pl.ds(0, n - 1)]
    pltpu.make_async_copy(others, others, recv_sem).wait()
    pltpu.make_async_copy(others, others, send_sem).wait()


def exchange(x, ident):
    sizes = (lax.axis_size("row"), lax.axis_size("col"))
    return pl.pallas_call(
        functools.partial(exchange_kernel, *sizes),
        out_shape=jax.ShapeDtypeStruct(x.shape, x.dtype),
        in_specs=[pl.BlockSpec(memory_space=pltpu.VMEM)],
        out_specs=pl.BlockSpec(memory_space=pltpu.VMEM),
        scratch_shapes=[pltpu.SemaphoreType.DMA, pltpu.SemaphoreType.DMA],
        compiler_params=pltpu.CompilerParams(collective_id=ident, has_side_effects=True),
        name=f"exchange_{ident}",
    )(x)


def per_device(
    pair,
    cotangent,
    length,
    norm_gain,
    norm_bias,
    left_weight,
    right_weight,
    gate_weight,
    out_gain,
    out_bias,
    out_weight,
):
    n_row = lax.axis_size("row")
    n_col = lax.axis_size("col")
    n = n_row * n_col
    rows, cols = pair.shape[:2]
    tokens = rows * n_row
    hidden = out_weight.shape[0]
    row_at = lax.axis_index("row") * rows
    col_at = lax.axis_index("col") * cols
    first_ok = row_at + jnp.arange(rows, dtype=jnp.int32) < length[0]
    second_ok = col_at + jnp.arange(cols, dtype=jnp.int32) < length[0]
    mask = (first_ok[:, None] & second_ok[None, :]).astype(jnp.float32).reshape(1, -1)

    def to_owner(tiles):
        return exchange(jnp.stack([t.reshape(n, rows * cols // 128, 128) for t in tiles], axis=1), 0)

    def whole(received):
        return received.reshape(n_row, n_col, rows, cols).transpose(0, 2, 1, 3).reshape(tokens, tokens)

    def tiled(matrix):
        t = matrix.reshape(n_row, rows, n_col, cols).transpose(0, 2, 1, 3)
        return t.reshape(n, rows * cols // 128, 128)

    pair_hat, pair_scale = normalize(pair.astype(jnp.float32))
    normed = (pair_hat * norm_gain + norm_bias).astype(jnp.bfloat16)
    flat = normed.reshape(rows * cols, -1)

    def dot(form, a, b):
        return jnp.einsum(form, a, b, preferred_element_type=jnp.float32)

    def gating(weight):
        projected = dot("pc,ch->hp", flat, weight)
        values = projected[:hidden]
        sig = jax.nn.sigmoid(projected[hidden:])
        return (mask * sig * values).astype(jnp.bfloat16), values, sig

    left, left_val, left_sig = gating(left_weight)
    right, right_val, right_sig = gating(right_weight)
    got = to_owner([left, right])
    big_l = whole(got[:, 0])
    big_r = whole(got[:, 1])
    tri_own = dot("ik,jk->ij", big_l, big_r).astype(jnp.bfloat16)
    tri = exchange(tiled(tri_own), 1).reshape(hidden, -1).astype(jnp.float32)
    center = tri - jnp.mean(tri, axis=0, keepdims=True)
    tri_scale = lax.rsqrt(jnp.mean(center * center, axis=0, keepdims=True) + EPS)
    tri_hat = center * tri_scale
    tri_normed = (tri_hat * out_gain[:, None] + out_bias[:, None]).astype(jnp.bfloat16)
    outer = dot("hp,hc->cp", tri_normed, out_weight)
    gate = jax.nn.sigmoid(dot("pc,cd->dp", flat, gate_weight))
    update = (gate * outer).astype(jnp.bfloat16).T.reshape(pair.shape)
    upstream = cotangent.reshape(rows * cols, -1).T.astype(jnp.float32)
    outer_grad = (upstream * gate).astype(jnp.bfloat16)
    gate_grad = (upstream * outer * gate * (1.0 - gate)).astype(jnp.bfloat16)
    grad_output = dot("hp,cp->hc", tri_normed, outer_grad)
    grad_gating = dot("pc,dp->cd", flat, gate_grad)
    tnorm_grad = dot("cp,hc->hp", outer_grad, out_weight)
    hat_grad = tnorm_grad * out_gain[:, None]
    tri_grad = (
        tri_scale
        * (
            hat_grad
            - jnp.mean(hat_grad, axis=0, keepdims=True)
            - tri_hat * jnp.mean(hat_grad * tri_hat, axis=0, keepdims=True)
        )
    ).astype(jnp.bfloat16)
    g = whole(exchange(tri_grad.reshape(n, rows * cols // 128, 128), 2))
    row_own = dot("ij,jk->ik", g, big_r).astype(jnp.bfloat16)
    col_own = dot("ij,ik->jk", g, big_l).astype(jnp.bfloat16)
    back = exchange(jnp.stack([tiled(row_own), tiled(col_own)], axis=1), 3)
    row_part = back[:, 0].reshape(hidden, -1).astype(jnp.float32)
    col_part = back[:, 1].reshape(hidden, -1).astype(jnp.float32)

    def push_back(part, values, sig, weight):
        comb = jnp.concatenate(
            [part * mask * sig, part * mask * values * sig * (1.0 - sig)], axis=0
        ).astype(jnp.bfloat16)
        return dot("hp,ch->pc", comb, weight), dot("pc,hp->ch", flat, comb)

    from_rows, grad_left = push_back(row_part, left_val, left_sig, left_weight)
    from_cols, grad_right = push_back(col_part, right_val, right_sig, right_weight)
    gate_back = dot("dp,cd->pc", gate_grad, gate_weight)
    normed_grad = (gate_back + from_rows + from_cols).reshape(pair.shape)
    scaled = normed_grad * norm_gain
    grad_pair = (
        pair_scale
        * (
            scaled
            - jnp.mean(scaled, axis=-1, keepdims=True)
            - pair_hat * jnp.mean(scaled * pair_hat, axis=-1, keepdims=True)
        )
    ).astype(jnp.bfloat16)
    grad_norms = jnp.stack(
        [
            jnp.sum(normed_grad * pair_hat, axis=(0, 1)),
            jnp.sum(normed_grad, axis=(0, 1)),
            jnp.sum(tnorm_grad * tri_hat, axis=1),
            jnp.sum(tnorm_grad, axis=1),
        ]
    )
    parts = [grad_left, grad_right, grad_gating, grad_output, grad_norms]
    flat_parts = jnp.concatenate([a.reshape(-1, 128) for a in parts], axis=0)
    size = flat_parts.shape[0]
    per = -(-size // (n * 8)) * 8
    padded = jnp.pad(flat_parts, ((0, per * n - size), (0, 0))).reshape(n, per, 128)
    mine = jnp.sum(exchange(padded, 4), axis=0) * (1.0 / tokens)
    total = exchange(jnp.broadcast_to(mine[None], (n,) + mine.shape), 5).reshape(n * per, 128)
    done, at = [], 0
    for a in parts:
        count = a.size // 128
        done.append(total[at : at + count].reshape(a.shape))
        at += count
    return (update, grad_pair, *done)


def solution(mesh):
    return jax.shard_map(
        per_device,
        mesh=mesh,
        in_specs=(P("row", "col", None), P("row", "col", None)) + (P(),) * 9,
        out_specs=(P("row", "col", None), P("row", "col", None)) + (P(),) * 5,
        check_vma=False,
    )
```

```python
import functools

import jax
import jax.numpy as jnp
from jax import lax
from jax.experimental import pallas as pl
from jax.experimental.pallas import tpu as pltpu
from jax.sharding import PartitionSpec as P

EPS = 1e-05
MESH = pl.DeviceIdType.MESH
BF = jnp.bfloat16
F32 = jnp.float32
LANES = 128
GROUP = 4


def dot(a, b):
    return jnp.dot(a, b, preferred_element_type=F32)


def dot_last(a, b):
    return lax.dot_general(a, b, (((1,), (1,)), ((), ())), preferred_element_type=F32)


def dot_first(a, b):
    return lax.dot_general(a, b, (((0,), (0,)), ((), ())), preferred_element_type=F32)


def center_scale(values):
    center = values - jnp.mean(values, axis=0, keepdims=True)
    inverse = lax.rsqrt(jnp.mean(center * center, axis=0, keepdims=True) + EPS)
    return center * inverse, inverse


def norm_back(grad, hat, scale):
    mean = jnp.mean(grad, axis=0, keepdims=True)
    along = jnp.mean(grad * hat, axis=0, keepdims=True)
    return scale * (grad - mean - hat * along)


def halves(a, b):
    half = a.shape[1] // 2
    first = lax.broadcasted_iota(jnp.int32, a.shape, 1) < half
    return (
        jnp.where(first, a, pltpu.roll(b, half, 1)),
        jnp.where(first, pltpu.roll(a, half, 1), b),
    )


def column(row_ref):
    return jnp.transpose(jnp.broadcast_to(row_ref[...], (LANES, LANES)))[:, :1]


def kernel(
    n_row,
    n_col,
    pair,
    cotangent,
    length,
    norm_gain,
    norm_bias,
    left_weight,
    right_weight,
    gate_weight,
    out_gain,
    out_bias,
    out_weight,
    update,
    grad_pair,
    grad_left,
    grad_right,
    grad_gating,
    grad_output,
    grad_norms,
    stage,
    hat_s,
    scale_s,
    normed_s,
    coef_s,
    gate_s,
    tnormed_s,
    ograd_s,
    ggrad_s,
    back_s,
    comb_s,
    big_l,
    big_r,
    big_g,
    send_a,
    recv_a,
    send_b,
    recv_b,
    send_c,
    recv_c,
    send_d,
    recv_d,
    send_e,
    recv_e,
    send_f,
    recv_f,
    send_sem,
    recv_sem,
):
    n = n_row * n_col
    rows, cols, chan = pair.shape
    hidden = out_weight.shape[0]
    blocks = rows * cols // LANES
    apart = LANES // cols * 8
    del apart
    tokens = n_row * rows
    half = rows // 2
    wide = GROUP * LANES
    row = lax.axis_index("row")
    col = lax.axis_index("col")
    me = row * n_col + col

    def coords(p):
        return (p // n_col, lax.rem(p, n_col))

    barrier = pltpu.get_barrier_semaphore()

    def greet(d, carry):
        peer = lax.rem(me + d, n)
        pl.semaphore_signal(barrier, inc=1, device_id=coords(peer), device_id_type=MESH)
        return carry

    def start_all(phase, src, dst, same=False):
        def send(d, carry):
            peer = lax.rem(me + d, n)
            pltpu.make_async_remote_copy(
                src_ref=src if same else src.at[peer],
                dst_ref=dst.at[me],
                send_sem=send_sem.at[phase],
                recv_sem=recv_sem.at[phase],
                device_id=coords(peer),
                device_id_type=MESH,
            ).start()
            return carry

        lax.fori_loop(1, n, send, 0)
        dst[me] = src[...] if same else src[me]

    def wait_on(sems, phase, dst):
        others = dst.at[pl.ds(0, n - 1)]
        pltpu.make_async_copy(others, others, sems.at[phase]).wait()

    def pack(dst, count, stride):
        def body(h, carry):
            at = pl.multiple_of(h * stride, 8)
            dst[h] = stage[pl.ds(at, count), :].astype(BF)
            return carry

        lax.fori_loop(0, n, body, 0, unroll=8)

    def unpack(src, count, stride):
        def body(h, carry):
            at = pl.multiple_of(h * stride, 8)
            stage[pl.ds(at, count), :] = src[h].astype(F32)
            return carry

        lax.fori_loop(0, n, body, 0, unroll=8)

    def spread(values, first, stride):
        for t in range(values.shape[1] // LANES):
            stage[pl.ds(first + t, LANES, stride=stride), :] = values[:, t * LANES : (t + 1) * LANES]

    def collect(first, stride, count):
        return jnp.concatenate(
            [stage[pl.ds(first + t, LANES, stride=stride), :] for t in range(count)], axis=1
        )

    def channels_first(ref, first):
        parts = []
        for t in range(GROUP):
            block = jnp.concatenate([ref[first + t], ref[first + t + half]], axis=0)
            parts.append(jnp.transpose(block.astype(F32)))
        return jnp.concatenate(parts, axis=1)

    def positions_first(ref, first, values):
        for t in range(GROUP):
            block = jnp.transpose(values[:, t * LANES : (t + 1) * LANES]).astype(BF)
            ref[first + t] = block[:cols]
            ref[first + t + half] = block[cols:]

    def lanes_at(first):
        return pl.ds(pl.multiple_of(first * LANES, LANES), wide)

    def assemble(src, at, dst):
        def body(r, carry):
            for q in range(n_col // 2):
                a = src[r * n_col + 2 * q, at : at + half, :].astype(F32)
                b = src[r * n_col + 2 * q + 1, at : at + half, :].astype(F32)
                low, high = halves(a, b)
                base = pl.multiple_of(r * rows, rows)
                dst[pl.ds(base, half), q * LANES : (q + 1) * LANES] = low.astype(BF)
                dst[pl.ds(base + half, half), q * LANES : (q + 1) * LANES] = high.astype(BF)
            return carry

        lax.fori_loop(0, n_row, body, 0, unroll=2)

    def disassemble(values, dst, at):
        for r in range(n_row):
            for q in range(n_col // 2):
                low = values[r * rows : r * rows + half, q * LANES : (q + 1) * LANES]
                high = values[r * rows + half : (r + 1) * rows, q * LANES : (q + 1) * LANES]
                a, b = halves(low, high)
                dst[r * n_col + 2 * q, at : at + half, :] = a.astype(BF)
                dst[r * n_col + 2 * q + 1, at : at + half, :] = b.astype(BF)

    lax.fori_loop(1, n, greet, 0)

    gain = column(norm_gain)
    bias = column(norm_bias)
    forward_weight = jnp.concatenate(
        [
            jnp.transpose(left_weight[...]),
            jnp.transpose(right_weight[...]),
            jnp.transpose(gate_weight[...]),
        ],
        axis=0,
    )

    def first_pass(g, carry):
        first = g * GROUP
        at = lanes_at(first)
        hat, scale = center_scale(channels_first(pair, first))
        normed = (hat * gain + bias).astype(BF)
        hat_s[:, at] = hat
        scale_s[:, at] = scale
        normed_s[:, at] = normed
        lane = lax.broadcasted_iota(jnp.int32, (1, wide), 1)
        inner = lax.rem(lane, LANES)
        i = row * rows + first + lane // LANES + inner // cols * half
        k = col * cols + lax.rem(inner, cols)
        real = length[0]
        mask = jnp.where((i < real) & (k < real), 1.0, 0.0).astype(F32)
        proj = dot(forward_weight, normed)
        for side in range(2):
            base = 2 * hidden * side
            sig = mask * jax.nn.sigmoid(proj[base + hidden : base + 2 * hidden])
            act = sig * proj[base : base + hidden]
            coef_s[2 * side, :, at] = sig
            coef_s[2 * side + 1, :, at] = act * (1.0 - sig)
            spread(act, first + side * blocks, 40)
        gate_s[:, at] = jax.nn.sigmoid(proj[4 * hidden :])
        return carry

    lax.fori_loop(0, blocks // GROUP, first_pass, 0)
    pack(send_a, 2 * blocks, 40)
    pl.semaphore_wait(barrier, n - 1)
    start_all(0, send_a, recv_a)

    wait_on(recv_sem, 0, recv_a)
    assemble(recv_a, 0, big_l)
    assemble(recv_a, blocks, big_r)
    disassemble(dot_last(big_l[...], big_r[...]), send_b, 0)
    start_all(1, send_b, recv_b)

    o_gain = column(out_gain)
    o_bias = column(out_bias)
    out_back = out_weight[...]
    out_forward = jnp.transpose(out_back)
    wait_on(recv_sem, 1, recv_b)
    unpack(recv_b, blocks, 24)

    def second_pass(g, carry):
        first = g * GROUP
        at = lanes_at(first)
        hat, scale = center_scale(collect(first, 24, GROUP))
        tri_normed = (hat * o_gain + o_bias).astype(BF)
        tnormed_s[:, at] = tri_normed
        outer = dot(out_forward, tri_normed)
        gate = gate_s[:, at]
        gated = gate * outer
        positions_first(update, first, gated)
        upstream = channels_first(cotangent, first)
        outer_grad = (upstream * gate).astype(BF)
        ograd_s[:, at] = outer_grad
        ggrad_s[:, at] = (upstream * gated * (1.0 - gate)).astype(BF)
        tnorm_grad = dot(out_back, outer_grad)
        spread(norm_back(tnorm_grad * o_gain, hat, scale), first, 24)
        along = tnorm_grad * hat
        return (
            carry[0] + jnp.sum(along, axis=1, keepdims=True),
            carry[1] + jnp.sum(tnorm_grad, axis=1, keepdims=True),
        )

    zero = jnp.zeros((hidden, 1), F32)
    o_gain_grad, o_bias_grad = lax.fori_loop(0, blocks // GROUP, second_pass, (zero, zero))
    pack(send_c, blocks, 24)
    start_all(2, send_c, recv_c)
    back_s[...] = dot(gate_weight[...], ggrad_s[...])
    part_output = dot_last(tnormed_s[...], ograd_s[...])
    part_gating = dot_last(normed_s[...], ggrad_s[...])

    wait_on(recv_sem, 2, recv_c)
    assemble(recv_c, 0, big_g)
    disassemble(dot(big_g[...], big_r[...]), send_d, 0)
    disassemble(dot_first(big_g[...], big_l[...]), send_d, blocks)
    start_all(3, send_d, recv_d)

    backward_weight = jnp.concatenate([left_weight[...], right_weight[...]], axis=1)
    wait_on(recv_sem, 3, recv_d)
    unpack(recv_d, 2 * blocks, 40)

    def third_pass(g, carry):
        first = g * GROUP
        at = lanes_at(first)
        from_row = collect(first, 40, GROUP)
        from_col = collect(first + blocks, 40, GROUP)
        comb = jnp.concatenate(
            [
                from_row * coef_s[0, :, at],
                from_row * coef_s[1, :, at],
                from_col * coef_s[2, :, at],
                from_col * coef_s[3, :, at],
            ],
            axis=0,
        ).astype(BF)
        comb_s[:, at] = comb
        normed_grad = back_s[:, at] + dot(backward_weight, comb)
        back_s[:, at] = normed_grad
        along = normed_grad * hat_s[:, at]
        return (
            carry[0] + jnp.sum(along, axis=1, keepdims=True),
            carry[1] + jnp.sum(normed_grad, axis=1, keepdims=True),
        )

    gain_grad, bias_grad = lax.fori_loop(0, blocks // GROUP, third_pass, (zero, zero))
    spread(dot_last(normed_s[...], comb_s[...]), 0, 24)
    spread(part_gating, 4, 24)
    spread(part_output, 5, 24)
    lane = lax.broadcasted_iota(jnp.int32, (LANES, LANES), 1)
    norms = jnp.where(lane == 0, gain_grad, 0.0)
    norms = jnp.where(lane == 1, bias_grad, norms)
    norms = jnp.where(lane == 2, o_gain_grad, norms)
    norms = jnp.where(lane == 3, o_bias_grad, norms)
    spread(norms, 6, 24)
    spread(jnp.zeros_like(norms), 7, 24)
    pack(send_e, 8, 24)
    start_all(4, send_e, recv_e)

    def fourth_pass(g, carry):
        first = g * GROUP
        at = lanes_at(first)
        grad = norm_back(back_s[:, at] * gain, hat_s[:, at], scale_s[:, at])
        positions_first(grad_pair, first, grad)
        return carry

    lax.fori_loop(0, blocks // GROUP, fourth_pass, 0)

    wait_on(recv_sem, 4, recv_e)

    def add(p, total):
        return total + recv_e[p].astype(F32)

    total = lax.fori_loop(0, n, add, jnp.zeros((8, LANES), F32), unroll=8)
    send_f[...] = (total * (1.0 / tokens)).astype(BF)
    start_all(5, send_f, recv_f, same=True)
    wait_on(recv_sem, 5, recv_f)
    unpack(recv_f, 8, 24)
    grad_left[...] = collect(0, 24, 2)
    grad_right[...] = collect(2, 24, 2)
    grad_gating[...] = collect(4, 24, 1)
    grad_output[...] = collect(5, 24, 1)
    grad_norms[...] = jnp.transpose(collect(6, 24, 1))[:4]
    for phase, dst in enumerate((recv_a, recv_b, recv_c, recv_d, recv_e, recv_f)):
        wait_on(send_sem, phase, dst)


def per_device(pair, cotangent, length, *weights):
    n_row = lax.axis_size("row")
    n_col = lax.axis_size("col")
    n = n_row * n_col
    rows, cols, chan = pair.shape
    hidden = weights[-1].shape[0]
    tokens = n_row * rows
    places = rows * cols
    blocks = places // LANES
    weights = [w.reshape(1, -1) if w.ndim == 1 else w for w in weights]
    vmem = pl.BlockSpec(memory_space=pltpu.VMEM)
    smem = pl.BlockSpec(memory_space=pltpu.SMEM)
    shape = jax.ShapeDtypeStruct
    return pl.pallas_call(
        functools.partial(kernel, n_row, n_col),
        out_shape=(
            shape(pair.shape, BF),
            shape(pair.shape, BF),
            shape((chan, 2 * hidden), F32),
            shape((chan, 2 * hidden), F32),
            shape((chan, chan), F32),
            shape((hidden, chan), F32),
            shape((4, chan), F32),
        ),
        in_specs=[vmem, vmem, smem] + [vmem] * len(weights),
        out_specs=(vmem,) * 7,
        scratch_shapes=[
            pltpu.VMEM((n * 40, LANES), F32),
            pltpu.VMEM((chan, places), F32),
            pltpu.VMEM((1, places), F32),
            pltpu.VMEM((chan, places), BF),
            pltpu.VMEM((4, hidden, places), F32),
            pltpu.VMEM((chan, places), F32),
            pltpu.VMEM((hidden, places), BF),
            pltpu.VMEM((chan, places), BF),
            pltpu.VMEM((chan, places), BF),
            pltpu.VMEM((chan, places), F32),
            pltpu.VMEM((4 * hidden, places), BF),
            pltpu.VMEM((tokens, tokens), BF),
            pltpu.VMEM((tokens, tokens), BF),
            pltpu.VMEM((tokens, tokens), BF),
            pltpu.VMEM((n, 2 * blocks, LANES), BF),
            pltpu.VMEM((n, 2 * blocks, LANES), BF),
            pltpu.VMEM((n, blocks, LANES), BF),
            pltpu.VMEM((n, blocks, LANES), BF),
            pltpu.VMEM((n, blocks, LANES), BF),
            pltpu.VMEM((n, blocks, LANES), BF),
            pltpu.VMEM((n, 2 * blocks, LANES), BF),
            pltpu.VMEM((n, 2 * blocks, LANES), BF),
            pltpu.VMEM((n, 8, LANES), BF),
            pltpu.VMEM((n, 8, LANES), BF),
            pltpu.VMEM((8, LANES), BF),
            pltpu.VMEM((n, 8, LANES), BF),
            pltpu.SemaphoreType.DMA((6,)),
            pltpu.SemaphoreType.DMA((6,)),
        ],
        compiler_params=pltpu.CompilerParams(
            collective_id=0, has_side_effects=True, vmem_limit_bytes=56 << 20
        ),
        name="triangle",
    )(pair, cotangent, length, *weights)


def solution(mesh):
    return jax.shard_map(
        per_device,
        mesh=mesh,
        in_specs=(P("row", "col", None), P("row", "col", None)) + (P(),) * 9,
        out_specs=(P("row", "col", None), P("row", "col", None)) + (P(),) * 5,
        check_vma=False,
    )
```

```python
import functools

import jax
import jax.numpy as jnp
from jax import lax
from jax.experimental import pallas as pl
from jax.experimental.pallas import tpu as pltpu
from jax.sharding import PartitionSpec as P

EPS = 1e-05
MESH = pl.DeviceIdType.MESH
BF = jnp.bfloat16
F32 = jnp.float32
LANES = 128
GROUP = 4


def dot(a, b):
    return jnp.dot(a, b, preferred_element_type=F32)


def dot_last(a, b):
    return lax.dot_general(a, b, (((1,), (1,)), ((), ())), preferred_element_type=F32)


def dot_first(a, b):
    return lax.dot_general(a, b, (((0,), (0,)), ((), ())), preferred_element_type=F32)


def center_scale(values):
    center = values - jnp.mean(values, axis=0, keepdims=True)
    inverse = lax.rsqrt(jnp.mean(center * center, axis=0, keepdims=True) + EPS)
    return center * inverse, inverse


def norm_back(grad, hat, scale):
    mean = jnp.mean(grad, axis=0, keepdims=True)
    along = jnp.mean(grad * hat, axis=0, keepdims=True)
    return scale * (grad - mean - hat * along)


def halves(a, b):
    half = a.shape[1] // 2
    first = lax.broadcasted_iota(jnp.int32, a.shape, 1) < half
    return (
        jnp.where(first, a, pltpu.roll(b, half, 1)),
        jnp.where(first, pltpu.roll(a, half, 1), b),
    )


def column(row_ref):
    return jnp.transpose(jnp.broadcast_to(row_ref[...], (LANES, LANES)))[:, :1]


def distance(step):
    return sum(min(d, 4 - d) for d in step[:3])


STEPS = [
    (dx, dy, dz, dc)
    for dx in range(4)
    for dy in range(4)
    for dz in range(4)
    for dc in range(2)
    if (dx, dy, dz, dc) != (0, 0, 0, 0)
]
STEPS.sort(key=lambda step: (-distance(step), step[3]))


def peers(row, col):
    z = row // 8 * 2 + lax.rem(col, 2)
    x = lax.rem(row // 2, 4)
    core = lax.rem(row, 2)
    y = col // 2
    at_x = [lax.rem(x + d, 4) * 2 for d in range(4)]
    at_y = [lax.rem(y + d, 4) * 2 for d in range(4)]
    at_z = [lax.rem(z + d, 4) for d in range(4)]
    high = [q // 2 * 8 for q in at_z]
    low = [lax.rem(q, 2) for q in at_z]
    at_core = [core, 1 - core]
    found = []
    for dx, dy, dz, dc in STEPS:
        to_row = high[dz] + at_x[dx] + at_core[dc]
        to_col = at_y[dy] + low[dz]
        found.append((to_row, to_col, to_row * 8 + to_col))
    return found


def kernel(
    n_row,
    n_col,
    pair_hbm,
    cotangent_hbm,
    length,
    *refs,
):
    weights_hbm, refs = refs[:8], refs[8:]
    kernel_body(n_row, n_col, pair_hbm, cotangent_hbm, length, weights_hbm, *refs)


def kernel_body(
    n_row,
    n_col,
    pair_hbm,
    cotangent_hbm,
    length,
    weights_hbm,
    update,
    grad_pair,
    recv_f,
    pair,
    norm_gain,
    norm_bias,
    left_weight,
    right_weight,
    gate_weight,
    cotangent,
    out_gain,
    out_bias,
    out_weight,
    stage,
    hat_s,
    scale_s,
    normed_s,
    coef_s,
    gate_s,
    tnormed_s,
    ograd_s,
    ggrad_s,
    back_s,
    comb_s,
    big_l,
    big_r,
    big_g,
    send_a,
    recv_a,
    send_b,
    recv_b,
    send_c,
    recv_c,
    send_d,
    recv_d,
    send_e,
    recv_e,
    send_f,
    send_sem,
    recv_sem,
    load_sem,
):
    n = n_row * n_col
    rows, cols, chan = pair.shape
    hidden = out_weight.shape[0]
    blocks = rows * cols // LANES
    tokens = n_row * rows
    half = rows // 2
    wide = GROUP * LANES
    row = lax.axis_index("row")
    col = lax.axis_index("col")
    me = row * n_col + col

    early = (pair, norm_gain, norm_bias, left_weight, right_weight, gate_weight)
    late = (cotangent, out_gain, out_bias, out_weight)
    sources = (pair_hbm, *weights_hbm[:5], cotangent_hbm, *weights_hbm[5:])
    loads = [
        pltpu.make_async_copy(src, dst, load_sem.at[t])
        for t, (src, dst) in enumerate(zip(sources, early + late))
    ]
    for load in loads:
        load.start()
    barrier = pltpu.get_barrier_semaphore()
    others = peers(row, col)
    for to_row, to_col, _ in others:
        pl.semaphore_signal(barrier, inc=1, device_id=(to_row, to_col), device_id_type=MESH)

    def start_all(phase, src, dst, same=False):
        for to_row, to_col, peer in others:
            pltpu.make_async_remote_copy(
                src_ref=src if same else src.at[peer],
                dst_ref=dst.at[me],
                send_sem=send_sem.at[phase],
                recv_sem=recv_sem.at[phase],
                device_id=(to_row, to_col),
                device_id_type=MESH,
            ).start()
        dst[me] = src[...] if same else src[me]

    def wait_on(sems, phase, dst):
        part = dst.at[pl.ds(0, n - 1)]
        pltpu.make_async_copy(part, part, sems.at[phase]).wait()

    def pack(dst, count, stride):
        def body(h, carry):
            at = pl.multiple_of(h * stride, 8)
            dst[h] = stage[pl.ds(at, count), :].astype(BF)
            return carry

        lax.fori_loop(0, n, body, 0, unroll=8)

    def unpack(src, count, stride):
        def body(h, carry):
            at = pl.multiple_of(h * stride, 8)
            stage[pl.ds(at, count), :] = src[h].astype(F32)
            return carry

        lax.fori_loop(0, n, body, 0, unroll=8)

    def spread(values, first, stride):
        for t in range(values.shape[1] // LANES):
            stage[pl.ds(first + t, LANES, stride=stride), :] = values[:, t * LANES : (t + 1) * LANES]

    def collect(first, stride, count):
        return jnp.concatenate(
            [stage[pl.ds(first + t, LANES, stride=stride), :] for t in range(count)], axis=1
        )

    def channels_first(ref, first):
        parts = []
        for t in range(GROUP):
            block = jnp.concatenate([ref[first + t], ref[first + t + half]], axis=0)
            parts.append(jnp.transpose(block.astype(F32)))
        return jnp.concatenate(parts, axis=1)

    def positions_first(ref, first, values):
        for t in range(GROUP):
            block = jnp.transpose(values[:, t * LANES : (t + 1) * LANES]).astype(BF)
            ref[first + t] = block[:cols]
            ref[first + t + half] = block[cols:]

    def lanes_at(first):
        return pl.ds(pl.multiple_of(first * LANES, LANES), wide)

    def assemble(src, at, dst):
        def body(r, carry):
            for q in range(n_col // 2):
                a = src[r * n_col + 2 * q, at : at + half, :].astype(F32)
                b = src[r * n_col + 2 * q + 1, at : at + half, :].astype(F32)
                low, high = halves(a, b)
                base = pl.multiple_of(r * rows, rows)
                dst[pl.ds(base, half), q * LANES : (q + 1) * LANES] = low.astype(BF)
                dst[pl.ds(base + half, half), q * LANES : (q + 1) * LANES] = high.astype(BF)
            return carry

        lax.fori_loop(0, n_row, body, 0, unroll=2)

    def disassemble(values, dst, at):
        for r in range(n_row):
            for q in range(n_col // 2):
                low = values[r * rows : r * rows + half, q * LANES : (q + 1) * LANES]
                high = values[r * rows + half : (r + 1) * rows, q * LANES : (q + 1) * LANES]
                a, b = halves(low, high)
                dst[r * n_col + 2 * q, at : at + half, :] = a.astype(BF)
                dst[r * n_col + 2 * q + 1, at : at + half, :] = b.astype(BF)

    for load in loads[: len(early)]:
        load.wait()
    gain = column(norm_gain)
    bias = column(norm_bias)
    forward_weight = jnp.concatenate(
        [
            jnp.transpose(left_weight[...]),
            jnp.transpose(right_weight[...]),
            jnp.transpose(gate_weight[...]),
        ],
        axis=0,
    )

    def first_pass(g, carry):
        first = g * GROUP
        at = lanes_at(first)
        hat, scale = center_scale(channels_first(pair, first))
        normed = (hat * gain + bias).astype(BF)
        hat_s[:, at] = hat
        scale_s[:, at] = scale
        normed_s[:, at] = normed
        lane = lax.broadcasted_iota(jnp.int32, (1, wide), 1)
        inner = lax.rem(lane, LANES)
        i = row * rows + first + lane // LANES + inner // cols * half
        k = col * cols + lax.rem(inner, cols)
        real = length[0]
        mask = jnp.where((i < real) & (k < real), 1.0, 0.0).astype(F32)
        proj = dot(forward_weight, normed)
        for side in range(2):
            base = 2 * hidden * side
            sig = mask * jax.nn.sigmoid(proj[base + hidden : base + 2 * hidden])
            act = sig * proj[base : base + hidden]
            coef_s[2 * side, :, at] = sig
            coef_s[2 * side + 1, :, at] = act * (1.0 - sig)
            spread(act, first + side * blocks, 40)
        gate_s[:, at] = jax.nn.sigmoid(proj[4 * hidden :])
        return carry

    lax.fori_loop(0, blocks // GROUP, first_pass, 0)
    pack(send_a, 2 * blocks, 40)
    pl.semaphore_wait(barrier, n - 1)
    start_all(0, send_a, recv_a)

    wait_on(recv_sem, 0, recv_a)
    assemble(recv_a, 0, big_l)
    assemble(recv_a, blocks, big_r)
    disassemble(dot_last(big_l[...], big_r[...]), send_b, 0)
    start_all(1, send_b, recv_b)

    for load in loads[len(early) :]:
        load.wait()
    o_gain = column(out_gain)
    o_bias = column(out_bias)
    out_back = out_weight[...]
    out_forward = jnp.transpose(out_back)
    wait_on(recv_sem, 1, recv_b)
    unpack(recv_b, blocks, 24)

    def second_pass(g, carry):
        first = g * GROUP
        at = lanes_at(first)
        hat, scale = center_scale(collect(first, 24, GROUP))
        tri_normed = (hat * o_gain + o_bias).astype(BF)
        tnormed_s[:, at] = tri_normed
        outer = dot(out_forward, tri_normed)
        gate = gate_s[:, at]
        gated = gate * outer
        positions_first(update, first, gated)
        upstream = channels_first(cotangent, first)
        outer_grad = (upstream * gate).astype(BF)
        ograd_s[:, at] = outer_grad
        ggrad_s[:, at] = (upstream * gated * (1.0 - gate)).astype(BF)
        tnorm_grad = dot(out_back, outer_grad)
        spread(norm_back(tnorm_grad * o_gain, hat, scale), first, 24)
        along = tnorm_grad * hat
        return (
            carry[0] + jnp.sum(along, axis=1, keepdims=True),
            carry[1] + jnp.sum(tnorm_grad, axis=1, keepdims=True),
        )

    zero = jnp.zeros((hidden, 1), F32)
    o_gain_grad, o_bias_grad = lax.fori_loop(0, blocks // GROUP, second_pass, (zero, zero))
    pack(send_c, blocks, 24)
    start_all(2, send_c, recv_c)
    back_s[...] = dot(gate_weight[...], ggrad_s[...])
    part_output = dot_last(tnormed_s[...], ograd_s[...])
    part_gating = dot_last(normed_s[...], ggrad_s[...])

    wait_on(recv_sem, 2, recv_c)
    assemble(recv_c, 0, big_g)
    disassemble(dot(big_g[...], big_r[...]), send_d, 0)
    disassemble(dot_first(big_g[...], big_l[...]), send_d, blocks)
    start_all(3, send_d, recv_d)

    backward_weight = jnp.concatenate([left_weight[...], right_weight[...]], axis=1)
    wait_on(recv_sem, 3, recv_d)
    unpack(recv_d, 2 * blocks, 40)

    def third_pass(g, carry):
        first = g * GROUP
        at = lanes_at(first)
        from_row = collect(first, 40, GROUP)
        from_col = collect(first + blocks, 40, GROUP)
        comb = jnp.concatenate(
            [
                from_row * coef_s[0, :, at],
                from_row * coef_s[1, :, at],
                from_col * coef_s[2, :, at],
                from_col * coef_s[3, :, at],
            ],
            axis=0,
        ).astype(BF)
        comb_s[:, at] = comb
        normed_grad = back_s[:, at] + dot(backward_weight, comb)
        back_s[:, at] = normed_grad
        along = normed_grad * hat_s[:, at]
        return (
            carry[0] + jnp.sum(along, axis=1, keepdims=True),
            carry[1] + jnp.sum(normed_grad, axis=1, keepdims=True),
        )

    gain_grad, bias_grad = lax.fori_loop(0, blocks // GROUP, third_pass, (zero, zero))
    spread(dot_last(normed_s[...], comb_s[...]), 0, 24)
    spread(part_gating, 4, 24)
    spread(part_output, 5, 24)
    lane = lax.broadcasted_iota(jnp.int32, (LANES, LANES), 1)
    norms = jnp.where(lane == 0, gain_grad, 0.0)
    norms = jnp.where(lane == 1, bias_grad, norms)
    norms = jnp.where(lane == 2, o_gain_grad, norms)
    norms = jnp.where(lane == 3, o_bias_grad, norms)
    spread(norms, 6, 24)
    spread(jnp.zeros_like(norms), 7, 24)
    pack(send_e, 8, 24)
    start_all(4, send_e, recv_e)

    def fourth_pass(g, carry):
        first = g * GROUP
        at = lanes_at(first)
        grad = norm_back(back_s[:, at] * gain, hat_s[:, at], scale_s[:, at])
        positions_first(grad_pair, first, grad)
        return carry

    lax.fori_loop(0, blocks // GROUP, fourth_pass, 0)

    wait_on(recv_sem, 4, recv_e)

    def add(p, total):
        return total + recv_e[p].astype(F32)

    total = lax.fori_loop(0, n, add, jnp.zeros((8, LANES), F32), unroll=8)
    send_f[...] = (total * (1.0 / tokens)).astype(BF)
    start_all(5, send_f, recv_f, same=True)
    wait_on(recv_sem, 5, recv_f)
    for phase, dst in enumerate((recv_a, recv_b, recv_c, recv_d, recv_e, recv_f)):
        wait_on(send_sem, phase, dst)


def finish(
    update_in,
    grad_pair_in,
    totals,
    update,
    grad_pair,
    grad_left,
    grad_right,
    grad_gating,
    grad_output,
    grad_norms,
    stage,
    sems,
):
    stores = [
        pltpu.make_async_copy(update_in, update, sems.at[0]),
        pltpu.make_async_copy(grad_pair_in, grad_pair, sems.at[1]),
    ]
    for store in stores:
        store.start()

    def unpack(h, carry):
        at = pl.multiple_of(h * 24, 8)
        stage[pl.ds(at, 8), :] = totals[h].astype(F32)
        return carry

    lax.fori_loop(0, LANES, unpack, 0, unroll=8)

    def collect(first):
        return stage[pl.ds(first, LANES, stride=24), :]

    for t in range(2):
        grad_left[:, t * LANES : (t + 1) * LANES] = collect(t)
        grad_right[:, t * LANES : (t + 1) * LANES] = collect(2 + t)
    grad_gating[...] = collect(4)
    grad_output[...] = collect(5)
    grad_norms[...] = jnp.transpose(collect(6))[:4]
    for store in stores:
        store.wait()


def per_device(pair, cotangent, length, *weights):
    n_row = lax.axis_size("row")
    n_col = lax.axis_size("col")
    n = n_row * n_col
    rows, cols, chan = pair.shape
    hidden = weights[-1].shape[0]
    tokens = n_row * rows
    places = rows * cols
    blocks = places // LANES
    weights = [w.reshape(1, -1) if w.ndim == 1 else w for w in weights]
    vmem = pl.BlockSpec(memory_space=pltpu.VMEM)
    smem = pl.BlockSpec(memory_space=pltpu.SMEM)
    shape = jax.ShapeDtypeStruct
    hbm = pl.BlockSpec(memory_space=pl.ANY)
    far = functools.partial(pltpu.with_memory_space_constraint, memory_space=pltpu.HBM)
    raw = pl.pallas_call(
        functools.partial(kernel, n_row, n_col),
        out_shape=(
            pltpu.VMEM(pair.shape, BF),
            pltpu.VMEM(pair.shape, BF),
            pltpu.VMEM((n, 8, LANES), BF),
        ),
        in_specs=[hbm, hbm, smem] + [hbm] * len(weights),
        out_specs=(vmem,) * 3,
        scratch_shapes=[
            pltpu.VMEM(pair.shape, BF),
            *[pltpu.VMEM(w.shape, w.dtype) for w in weights[:5]],
            pltpu.VMEM(pair.shape, BF),
            *[pltpu.VMEM(w.shape, w.dtype) for w in weights[5:]],
            pltpu.VMEM((n * 40, LANES), F32),
            pltpu.VMEM((chan, places), F32),
            pltpu.VMEM((1, places), F32),
            pltpu.VMEM((chan, places), BF),
            pltpu.VMEM((4, hidden, places), F32),
            pltpu.VMEM((chan, places), F32),
            pltpu.VMEM((hidden, places), BF),
            pltpu.VMEM((chan, places), BF),
            pltpu.VMEM((chan, places), BF),
            pltpu.VMEM((chan, places), F32),
            pltpu.VMEM((4 * hidden, places), BF),
            pltpu.VMEM((tokens, tokens), BF),
            pltpu.VMEM((tokens, tokens), BF),
            pltpu.VMEM((tokens, tokens), BF),
            pltpu.VMEM((n, 2 * blocks, LANES), BF),
            pltpu.VMEM((n, 2 * blocks, LANES), BF),
            pltpu.VMEM((n, blocks, LANES), BF),
            pltpu.VMEM((n, blocks, LANES), BF),
            pltpu.VMEM((n, blocks, LANES), BF),
            pltpu.VMEM((n, blocks, LANES), BF),
            pltpu.VMEM((n, 2 * blocks, LANES), BF),
            pltpu.VMEM((n, 2 * blocks, LANES), BF),
            pltpu.VMEM((n, 8, LANES), BF),
            pltpu.VMEM((n, 8, LANES), BF),
            pltpu.VMEM((8, LANES), BF),
            pltpu.SemaphoreType.DMA((6,)),
            pltpu.SemaphoreType.DMA((6,)),
            pltpu.SemaphoreType.DMA((10,)),
        ],
        compiler_params=pltpu.CompilerParams(
            collective_id=0, has_side_effects=True, vmem_limit_bytes=40 << 20
        ),
        name="triangle",
    )(far(pair), far(cotangent), length, *[far(w) for w in weights])
    raw = [pltpu.with_memory_space_constraint(a, pltpu.VMEM) for a in raw]
    return pl.pallas_call(
        finish,
        out_shape=(
            shape(pair.shape, BF),
            shape(pair.shape, BF),
            shape((chan, 2 * hidden), F32),
            shape((chan, 2 * hidden), F32),
            shape((chan, chan), F32),
            shape((hidden, chan), F32),
            shape((4, chan), F32),
        ),
        in_specs=[vmem] * 3,
        out_specs=(hbm, hbm) + (vmem,) * 5,
        scratch_shapes=[pltpu.VMEM((LANES * 24, LANES), F32), pltpu.SemaphoreType.DMA((2,))],
        compiler_params=pltpu.CompilerParams(vmem_limit_bytes=8 << 20),
        name="finish",
    )(*raw)


def solution(mesh):
    return jax.shard_map(
        per_device,
        mesh=mesh,
        in_specs=(P("row", "col", None), P("row", "col", None)) + (P(),) * 9,
        out_specs=(P("row", "col", None), P("row", "col", None)) + (P(),) * 5,
        check_vma=False,
    )
```

```python
import functools

import jax
import jax.numpy as jnp
from jax import lax
from jax.experimental import pallas as pl
from jax.experimental.pallas import tpu as pltpu
from jax.sharding import PartitionSpec as P

EPS = 1e-05
MESH = pl.DeviceIdType.MESH
BF = jnp.bfloat16
F32 = jnp.float32
LANES = 128
GROUP = 4


def dot(a, b):
    return jnp.dot(a, b, preferred_element_type=F32)


def dot_last(a, b):
    return lax.dot_general(a, b, (((1,), (1,)), ((), ())), preferred_element_type=F32)


def dot_first(a, b):
    return lax.dot_general(a, b, (((0,), (0,)), ((), ())), preferred_element_type=F32)


def center_scale(values):
    center = values - jnp.mean(values, axis=0, keepdims=True)
    inverse = lax.rsqrt(jnp.mean(center * center, axis=0, keepdims=True) + EPS)
    return center * inverse, inverse


def norm_back(grad, hat, scale):
    mean = jnp.mean(grad, axis=0, keepdims=True)
    along = jnp.mean(grad * hat, axis=0, keepdims=True)
    return scale * (grad - mean - hat * along)


def halves(a, b):
    half = a.shape[1] // 2
    first = lax.broadcasted_iota(jnp.int32, a.shape, 1) < half
    return (
        jnp.where(first, a, pltpu.roll(b, half, 1)),
        jnp.where(first, pltpu.roll(a, half, 1), b),
    )


def column(row_ref):
    return jnp.transpose(jnp.broadcast_to(row_ref[...], (LANES, LANES)))[:, :1]


def distance(step):
    return sum(min(d, 4 - d) for d in step[:3])


STEPS = [
    (dx, dy, dz, dc)
    for dx in range(4)
    for dy in range(4)
    for dz in range(4)
    for dc in range(2)
    if (dx, dy, dz, dc) != (0, 0, 0, 0)
]
STEPS.sort(key=lambda step: (-distance(step), step[3]))


def peers(row, col):
    z = row // 8 * 2 + lax.rem(col, 2)
    x = lax.rem(row // 2, 4)
    core = lax.rem(row, 2)
    y = col // 2
    at_x = [lax.rem(x + d, 4) * 2 for d in range(4)]
    at_y = [lax.rem(y + d, 4) * 2 for d in range(4)]
    at_z = [lax.rem(z + d, 4) for d in range(4)]
    high = [q // 2 * 8 for q in at_z]
    low = [lax.rem(q, 2) for q in at_z]
    at_core = [core, 1 - core]
    found = []
    for dx, dy, dz, dc in STEPS:
        to_row = high[dz] + at_x[dx] + at_core[dc]
        to_col = at_y[dy] + low[dz]
        found.append((to_row, to_col, to_row * 8 + to_col))
    return found


def kernel(
    n_row,
    n_col,
    pair_hbm,
    cotangent_hbm,
    length,
    *refs,
):
    weights_hbm, refs = refs[:8], refs[8:]
    kernel_body(n_row, n_col, pair_hbm, cotangent_hbm, length, weights_hbm, *refs)


def kernel_body(
    n_row,
    n_col,
    pair_hbm,
    cotangent_hbm,
    length,
    weights_hbm,
    update,
    grad_pair,
    recv_f,
    pair,
    norm_gain,
    norm_bias,
    left_weight,
    right_weight,
    gate_weight,
    cotangent,
    out_gain,
    out_bias,
    out_weight,
    stage,
    hat_s,
    scale_s,
    normed_s,
    coef_s,
    gate_s,
    up_s,
    hgrad_s,
    that_s,
    tnormed_s,
    ograd_s,
    ggrad_s,
    back_s,
    comb_s,
    big_l,
    big_r,
    big_g,
    send_a,
    recv_a,
    send_l,
    recv_l,
    send_b,
    recv_b,
    send_c,
    recv_c,
    send_row,
    recv_row,
    send_col,
    recv_col,
    send_e,
    recv_e,
    send_f,
    send_sem,
    recv_sem,
    load_sem,
):
    n = n_row * n_col
    rows, cols, chan = pair.shape
    hidden = out_weight.shape[0]
    blocks = rows * cols // LANES
    tokens = n_row * rows
    half = rows // 2
    wide = GROUP * LANES
    part = blocks // 2
    groups = part // GROUP
    row = lax.axis_index("row")
    col = lax.axis_index("col")
    me = row * n_col + col

    early = (pair, norm_gain, norm_bias, left_weight, right_weight, gate_weight)
    late = (cotangent, out_gain, out_bias, out_weight)
    sources = (pair_hbm, *weights_hbm[:5], cotangent_hbm, *weights_hbm[5:])
    loads = [
        pltpu.make_async_copy(src, dst, load_sem.at[t])
        for t, (src, dst) in enumerate(zip(sources, early + late))
    ]
    for load in loads:
        load.start()
    barrier = pltpu.get_barrier_semaphore()
    others = peers(row, col)
    for to_row, to_col, _ in others:
        pl.semaphore_signal(barrier, inc=1, device_id=(to_row, to_col), device_id_type=MESH)

    def start_all(phase, src, dst, same=False):
        for to_row, to_col, peer in others:
            pltpu.make_async_remote_copy(
                src_ref=src if same else src.at[peer],
                dst_ref=dst.at[me],
                send_sem=send_sem.at[phase],
                recv_sem=recv_sem.at[phase],
                device_id=(to_row, to_col),
                device_id_type=MESH,
            ).start()
        dst[me] = src[...] if same else src[me]

    def wait_on(sems, phase, dst):
        blocks_of = dst.at[pl.ds(0, n - 1)]
        pltpu.make_async_copy(blocks_of, blocks_of, sems.at[phase]).wait()

    def pack(dst, count, stride, first=0):
        def body(h, carry):
            at = pl.multiple_of(h * stride + first, 8)
            dst[h] = stage[pl.ds(at, count), :].astype(BF)
            return carry

        lax.fori_loop(0, n, body, 0, unroll=8)

    def unpack(src, count, stride, first=0):
        def body(h, carry):
            at = pl.multiple_of(h * stride + first, 8)
            stage[pl.ds(at, count), :] = src[h].astype(F32)
            return carry

        lax.fori_loop(0, n, body, 0, unroll=8)

    def spread(values, first, stride):
        for t in range(values.shape[1] // LANES):
            stage[pl.ds(first + t, LANES, stride=stride), :] = values[:, t * LANES : (t + 1) * LANES]

    def collect(first, stride, count):
        return jnp.concatenate(
            [stage[pl.ds(first + t, LANES, stride=stride), :] for t in range(count)], axis=1
        )

    def channels_first(ref, first):
        parts = []
        for t in range(GROUP):
            block = jnp.concatenate([ref[first + t], ref[first + t + half]], axis=0)
            parts.append(jnp.transpose(block.astype(F32)))
        return jnp.concatenate(parts, axis=1)

    def positions_first(ref, first, values):
        for t in range(GROUP):
            block = jnp.transpose(values[:, t * LANES : (t + 1) * LANES]).astype(BF)
            ref[first + t] = block[:cols]
            ref[first + t + half] = block[cols:]

    def lanes_at(first):
        return pl.ds(pl.multiple_of(first * LANES, LANES), wide)

    def assemble(src, at, count, dst):
        def body(r, carry):
            for q in range(n_col // 2):
                a = src[r * n_col + 2 * q, at : at + count, :].astype(F32)
                b = src[r * n_col + 2 * q + 1, at : at + count, :].astype(F32)
                both = jnp.concatenate(halves(a, b), axis=0).astype(BF)
                base = pl.multiple_of(r * 2 * count, 2 * count)
                dst[pl.ds(base, 2 * count), q * LANES : (q + 1) * LANES] = both
            return carry

        lax.fori_loop(0, n_row, body, 0, unroll=2)

    def disassemble(values, count, dst):
        for r in range(n_row):
            for q in range(n_col // 2):
                block = values[r * 2 * count : (r + 1) * 2 * count, q * LANES : (q + 1) * LANES]
                a, b = halves(block[:count], block[count:])
                dst[r * n_col + 2 * q] = a.astype(BF)
                dst[r * n_col + 2 * q + 1] = b.astype(BF)

    for load in loads[: len(early)]:
        load.wait()
    gain = column(norm_gain)
    bias = column(norm_bias)
    forward_weight = jnp.concatenate(
        [
            jnp.transpose(left_weight[...]),
            jnp.transpose(right_weight[...]),
            jnp.transpose(gate_weight[...]),
        ],
        axis=0,
    )

    def first_pass(g, carry):
        first = g * GROUP
        at = lanes_at(first)
        hat, scale = center_scale(channels_first(pair, first))
        normed = (hat * gain + bias).astype(BF)
        hat_s[:, at] = hat
        scale_s[:, at] = scale
        normed_s[:, at] = normed
        lane = lax.broadcasted_iota(jnp.int32, (1, wide), 1)
        inner = lax.rem(lane, LANES)
        i = row * rows + first + lane // LANES + inner // cols * half
        k = col * cols + lax.rem(inner, cols)
        real = length[0]
        mask = jnp.where((i < real) & (k < real), 1.0, 0.0).astype(F32)
        proj = dot(forward_weight, normed)
        for side in range(2):
            base = 2 * hidden * side
            sig = mask * jax.nn.sigmoid(proj[base + hidden : base + 2 * hidden])
            act = sig * proj[base : base + hidden]
            coef_s[2 * side, :, at] = sig
            coef_s[2 * side + 1, :, at] = act * (1.0 - sig)
            spread(act, first + (1 - side) * blocks, 40)
        gate_s[:, at] = jax.nn.sigmoid(proj[4 * hidden :])
        return carry

    lax.fori_loop(0, blocks // GROUP, first_pass, 0)
    pack(send_a, blocks + part, 40)
    pack(send_l, part, 40, blocks + part)
    pl.semaphore_wait(barrier, n - 1)
    start_all(0, send_a, recv_a)
    start_all(1, send_l, recv_l)

    for load in loads[len(early) :]:
        load.wait()
    o_gain = column(out_gain)
    o_bias = column(out_bias)
    out_back = out_weight[...]
    out_forward = jnp.transpose(out_back)
    zero = jnp.zeros((hidden, 1), F32)

    def early_pass(g, carry):
        first = g * GROUP
        at = lanes_at(first)
        upstream = channels_first(cotangent, first)
        up_s[:, at] = upstream.astype(BF)
        outer_grad = (upstream * gate_s[:, at]).astype(BF)
        ograd_s[:, at] = outer_grad
        tnorm_grad = dot(out_back, outer_grad)
        hgrad_s[:, at] = tnorm_grad
        return carry + jnp.sum(tnorm_grad, axis=1, keepdims=True)

    o_bias_grad = lax.fori_loop(0, blocks // GROUP, early_pass, zero)

    wait_on(recv_sem, 0, recv_a)
    assemble(recv_a, 0, blocks, big_r)
    assemble(recv_a, blocks, part, big_l.at[0])
    disassemble(dot_last(big_l[0], big_r[...]), part, send_b.at[0])
    start_all(2, send_b.at[0], recv_b.at[0])
    wait_on(recv_sem, 1, recv_l)
    assemble(recv_l, 0, part, big_l.at[1])
    disassemble(dot_last(big_l[1], big_r[...]), part, send_b.at[1])
    start_all(3, send_b.at[1], recv_b.at[1])

    for piece in range(2):
        wait_on(recv_sem, 2 + piece, recv_b.at[piece])
        unpack(recv_b.at[piece], part, 24)

        def second_pass(g, carry):
            first = g * GROUP
            at = lanes_at(piece * part + first)
            hat, scale = center_scale(collect(first, 24, GROUP))
            that_s[:, at] = hat
            spread(norm_back(hgrad_s[:, at] * o_gain, hat, scale), first, 24)
            return carry

        lax.fori_loop(0, groups, second_pass, 0)
        pack(send_c.at[piece], part, 24)
        start_all(4 + piece, send_c.at[piece], recv_c.at[piece])

    def late_pass(g, carry):
        first = g * GROUP
        at = lanes_at(first)
        hat = that_s[:, at]
        tri_normed = (hat * o_gain + o_bias).astype(BF)
        tnormed_s[:, at] = tri_normed
        gate = gate_s[:, at]
        gated = gate * dot(out_forward, tri_normed)
        positions_first(update, first, gated)
        ggrad_s[:, at] = (up_s[:, at].astype(F32) * gated * (1.0 - gate)).astype(BF)
        return carry + jnp.sum(hgrad_s[:, at] * hat, axis=1, keepdims=True)

    o_gain_grad = lax.fori_loop(0, blocks // GROUP, late_pass, zero)
    back_s[...] = dot(gate_weight[...], ggrad_s[...])
    part_output = dot_last(tnormed_s[...], ograd_s[...])
    part_gating = dot_last(normed_s[...], ggrad_s[...])

    for piece in range(2):
        wait_on(recv_sem, 4 + piece, recv_c.at[piece])
        here = pl.ds(piece * tokens // 2, tokens // 2)
        assemble(recv_c.at[piece], 0, part, big_g.at[here])
        disassemble(dot(big_g[here], big_r[...]), part, send_row.at[piece])
        start_all(6 + piece, send_row.at[piece], recv_row.at[piece])
    all_l = jnp.concatenate([big_l[0], big_l[1]], axis=0)
    disassemble(dot_first(big_g[...], all_l), blocks, send_col)
    start_all(8, send_col, recv_col)

    for piece in range(2):
        wait_on(recv_sem, 6 + piece, recv_row.at[piece])
        unpack(recv_row.at[piece], part, 24, piece * part)

    def through(weight, side, g):
        first = g * GROUP
        at = lanes_at(first)
        grad = collect(first, 24, GROUP)
        comb = jnp.concatenate(
            [grad * coef_s[2 * side, :, at], grad * coef_s[2 * side + 1, :, at]], axis=0
        ).astype(BF)
        comb_s[2 * hidden * side : 2 * hidden * (side + 1), at] = comb
        return at, back_s[:, at] + dot(weight[...], comb)

    def row_pass(g, carry):
        at, normed_grad = through(left_weight, 0, g)
        back_s[:, at] = normed_grad
        return carry

    def col_pass(g, carry):
        at, normed_grad = through(right_weight, 1, g)
        back_s[:, at] = normed_grad
        along = normed_grad * hat_s[:, at]
        return (
            carry[0] + jnp.sum(along, axis=1, keepdims=True),
            carry[1] + jnp.sum(normed_grad, axis=1, keepdims=True),
        )

    lax.fori_loop(0, blocks // GROUP, row_pass, 0)
    part_left = dot_last(normed_s[...], comb_s[: 2 * hidden])
    wait_on(recv_sem, 8, recv_col)
    unpack(recv_col, blocks, 24)
    gain_grad, bias_grad = lax.fori_loop(0, blocks // GROUP, col_pass, (zero, zero))
    spread(part_left, 0, 24)
    spread(dot_last(normed_s[...], comb_s[2 * hidden :]), 2, 24)
    spread(part_gating, 4, 24)
    spread(part_output, 5, 24)
    lane = lax.broadcasted_iota(jnp.int32, (LANES, LANES), 1)
    norms = jnp.where(lane == 0, gain_grad, 0.0)
    norms = jnp.where(lane == 1, bias_grad, norms)
    norms = jnp.where(lane == 2, o_gain_grad, norms)
    norms = jnp.where(lane == 3, o_bias_grad, norms)
    spread(norms, 6, 24)
    spread(jnp.zeros_like(norms), 7, 24)
    pack(send_e, 8, 24)
    start_all(9, send_e, recv_e)

    def fourth_pass(g, carry):
        first = g * GROUP
        at = lanes_at(first)
        grad = norm_back(back_s[:, at] * gain, hat_s[:, at], scale_s[:, at])
        positions_first(grad_pair, first, grad)
        return carry

    lax.fori_loop(0, blocks // GROUP, fourth_pass, 0)

    wait_on(recv_sem, 9, recv_e)

    def add(p, total):
        return total + recv_e[p].astype(F32)

    total = lax.fori_loop(0, n, add, jnp.zeros((8, LANES), F32), unroll=8)
    send_f[...] = (total * (1.0 / tokens)).astype(BF)
    start_all(10, send_f, recv_f, same=True)
    wait_on(recv_sem, 10, recv_f)
    halved = [dst.at[piece] for dst in (recv_b, recv_c, recv_row) for piece in range(2)]
    for phase, dst in enumerate((recv_a, recv_l, *halved, recv_col, recv_e, recv_f)):
        wait_on(send_sem, phase, dst)


def finish(
    update_in,
    grad_pair_in,
    totals,
    update,
    grad_pair,
    grad_left,
    grad_right,
    grad_gating,
    grad_output,
    grad_norms,
    stage,
    sems,
):
    stores = [
        pltpu.make_async_copy(update_in, update, sems.at[0]),
        pltpu.make_async_copy(grad_pair_in, grad_pair, sems.at[1]),
    ]
    for store in stores:
        store.start()

    def unpack(h, carry):
        at = pl.multiple_of(h * 24, 8)
        stage[pl.ds(at, 8), :] = totals[h].astype(F32)
        return carry

    lax.fori_loop(0, LANES, unpack, 0, unroll=8)

    def collect(first):
        return stage[pl.ds(first, LANES, stride=24), :]

    for t in range(2):
        grad_left[:, t * LANES : (t + 1) * LANES] = collect(t)
        grad_right[:, t * LANES : (t + 1) * LANES] = collect(2 + t)
    grad_gating[...] = collect(4)
    grad_output[...] = collect(5)
    grad_norms[...] = jnp.transpose(collect(6))[:4]
    for store in stores:
        store.wait()


def per_device(pair, cotangent, length, *weights):
    n_row = lax.axis_size("row")
    n_col = lax.axis_size("col")
    n = n_row * n_col
    rows, cols, chan = pair.shape
    hidden = weights[-1].shape[0]
    tokens = n_row * rows
    places = rows * cols
    blocks = places // LANES
    part = blocks // 2
    weights = [w.reshape(1, -1) if w.ndim == 1 else w for w in weights]
    vmem = pl.BlockSpec(memory_space=pltpu.VMEM)
    smem = pl.BlockSpec(memory_space=pltpu.SMEM)
    shape = jax.ShapeDtypeStruct
    hbm = pl.BlockSpec(memory_space=pl.ANY)
    far = functools.partial(pltpu.with_memory_space_constraint, memory_space=pltpu.HBM)
    raw = pl.pallas_call(
        functools.partial(kernel, n_row, n_col),
        out_shape=(
            pltpu.VMEM(pair.shape, BF),
            pltpu.VMEM(pair.shape, BF),
            pltpu.VMEM((n, 8, LANES), BF),
        ),
        in_specs=[hbm, hbm, smem] + [hbm] * len(weights),
        out_specs=(vmem,) * 3,
        scratch_shapes=[
            pltpu.VMEM(pair.shape, BF),
            *[pltpu.VMEM(w.shape, w.dtype) for w in weights[:5]],
            pltpu.VMEM(pair.shape, BF),
            *[pltpu.VMEM(w.shape, w.dtype) for w in weights[5:]],
            pltpu.VMEM((n * 40, LANES), F32),
            pltpu.VMEM((chan, places), F32),
            pltpu.VMEM((1, places), F32),
            pltpu.VMEM((chan, places), BF),
            pltpu.VMEM((4, hidden, places), F32),
            pltpu.VMEM((chan, places), F32),
            pltpu.VMEM((chan, places), BF),
            pltpu.VMEM((hidden, places), F32),
            pltpu.VMEM((hidden, places), F32),
            pltpu.VMEM((hidden, places), BF),
            pltpu.VMEM((chan, places), BF),
            pltpu.VMEM((chan, places), BF),
            pltpu.VMEM((chan, places), F32),
            pltpu.VMEM((4 * hidden, places), BF),
            pltpu.VMEM((2, tokens // 2, tokens), BF),
            pltpu.VMEM((tokens, tokens), BF),
            pltpu.VMEM((tokens, tokens), BF),
            *[pltpu.VMEM((n, blocks + part, LANES), BF)] * 2,
            *[pltpu.VMEM((n, part, LANES), BF)] * 2,
            *[pltpu.VMEM((2, n, part, LANES), BF)] * 6,
            *[pltpu.VMEM((n, blocks, LANES), BF)] * 2,
            *[pltpu.VMEM((n, 8, LANES), BF)] * 2,
            pltpu.VMEM((8, LANES), BF),
            pltpu.SemaphoreType.DMA((11,)),
            pltpu.SemaphoreType.DMA((11,)),
            pltpu.SemaphoreType.DMA((10,)),
        ],
        compiler_params=pltpu.CompilerParams(
            collective_id=0, has_side_effects=True, vmem_limit_bytes=40 << 20
        ),
        name="triangle",
    )(far(pair), far(cotangent), length, *[far(w) for w in weights])
    raw = [pltpu.with_memory_space_constraint(a, pltpu.VMEM) for a in raw]
    return pl.pallas_call(
        finish,
        out_shape=(
            shape(pair.shape, BF),
            shape(pair.shape, BF),
            shape((chan, 2 * hidden), F32),
            shape((chan, 2 * hidden), F32),
            shape((chan, chan), F32),
            shape((hidden, chan), F32),
            shape((4, chan), F32),
        ),
        in_specs=[vmem] * 3,
        out_specs=(hbm, hbm) + (vmem,) * 5,
        scratch_shapes=[pltpu.VMEM((LANES * 24, LANES), F32), pltpu.SemaphoreType.DMA((2,))],
        compiler_params=pltpu.CompilerParams(vmem_limit_bytes=8 << 20),
        name="finish",
    )(*raw)


def solution(mesh):
    return jax.shard_map(
        per_device,
        mesh=mesh,
        in_specs=(P("row", "col", None), P("row", "col", None)) + (P(),) * 9,
        out_specs=(P("row", "col", None), P("row", "col", None)) + (P(),) * 5,
        check_vma=False,
    )
```

```python
import functools

import jax
import jax.numpy as jnp
from jax import lax
from jax.experimental import pallas as pl
from jax.experimental.pallas import tpu as pltpu
from jax.sharding import PartitionSpec as P

EPS = 1e-05
MESH = pl.DeviceIdType.MESH
BF = jnp.bfloat16
F32 = jnp.float32
LANES = 128
GROUP = 8


def dot(a, b):
    return jnp.dot(a, b, preferred_element_type=F32)


def dot_last(a, b):
    return lax.dot_general(a, b, (((1,), (1,)), ((), ())), preferred_element_type=F32)


def dot_first(a, b):
    return lax.dot_general(a, b, (((0,), (0,)), ((), ())), preferred_element_type=F32)


def center_scale(values):
    center = values - jnp.mean(values, axis=0, keepdims=True)
    inverse = lax.rsqrt(jnp.mean(center * center, axis=0, keepdims=True) + EPS)
    return center * inverse, inverse


def norm_back(grad, hat, scale):
    mean = jnp.mean(grad, axis=0, keepdims=True)
    along = jnp.mean(grad * hat, axis=0, keepdims=True)
    return scale * (grad - mean - hat * along)


def halves(a, b):
    half = a.shape[1] // 2
    first = lax.broadcasted_iota(jnp.int32, a.shape, 1) < half
    return (
        jnp.where(first, a, pltpu.roll(b, half, 1)),
        jnp.where(first, pltpu.roll(a, half, 1), b),
    )


def column(row_ref):
    return jnp.transpose(jnp.broadcast_to(row_ref[...], (LANES, LANES)))[:, :1]


def distance(step):
    return sum(min(d, 4 - d) for d in step[:3])


STEPS = [
    (dx, dy, dz, dc)
    for dx in range(4)
    for dy in range(4)
    for dz in range(4)
    for dc in range(2)
    if (dx, dy, dz, dc) != (0, 0, 0, 0)
]
STEPS.sort(key=lambda step: (-distance(step), step[3]))


def peers(row, col):
    z = row // 8 * 2 + lax.rem(col, 2)
    x = lax.rem(row // 2, 4)
    core = lax.rem(row, 2)
    y = col // 2
    at_x = [lax.rem(x + d, 4) * 2 for d in range(4)]
    at_y = [lax.rem(y + d, 4) * 2 for d in range(4)]
    at_z = [lax.rem(z + d, 4) for d in range(4)]
    high = [q // 2 * 8 for q in at_z]
    low = [lax.rem(q, 2) for q in at_z]
    at_core = [core, 1 - core]
    found = []
    for dx, dy, dz, dc in STEPS:
        to_row = high[dz] + at_x[dx] + at_core[dc]
        to_col = at_y[dy] + low[dz]
        found.append((to_row, to_col, to_row * 8 + to_col))
    return found


def kernel(
    n_row,
    n_col,
    pair_hbm,
    cotangent_hbm,
    length,
    *refs,
):
    weights_hbm, refs = refs[:8], refs[8:]
    kernel_body(n_row, n_col, pair_hbm, cotangent_hbm, length, weights_hbm, *refs)


def kernel_body(
    n_row,
    n_col,
    pair_hbm,
    cotangent_hbm,
    length,
    weights_hbm,
    update,
    grad_pair,
    grad_left,
    grad_right,
    grad_gating,
    grad_output,
    grad_norms,
    pair,
    norm_gain,
    norm_bias,
    left_weight,
    right_weight,
    gate_weight,
    cotangent,
    out_gain,
    out_bias,
    out_weight,
    stage,
    hat_s,
    scale_s,
    normed_s,
    coef_s,
    gate_s,
    up_s,
    hgrad_s,
    that_s,
    tnormed_s,
    ograd_s,
    ggrad_s,
    back_s,
    comb_s,
    big_l,
    big_r,
    big_g,
    send_r,
    recv_r,
    send_l,
    recv_l,
    send_b,
    recv_b,
    send_c,
    recv_c,
    send_row,
    recv_row,
    send_col,
    recv_col,
    send_e,
    recv_e,
    send_h,
    recv_h,
    send_f,
    recv_f,
    send_g,
    recv_g,
    send_sem,
    recv_sem,
    load_sem,
):
    n = n_row * n_col
    rows, cols, chan = pair.shape
    hidden = out_weight.shape[0]
    blocks = rows * cols // LANES
    tokens = n_row * rows
    half = rows // 2
    wide = GROUP * LANES
    part = blocks // 2
    groups = part // GROUP
    row = lax.axis_index("row")
    col = lax.axis_index("col")
    me = row * n_col + col

    early = (pair, norm_gain, norm_bias, left_weight, right_weight, gate_weight)
    late = (cotangent, out_gain, out_bias, out_weight)
    sources = (pair_hbm, *weights_hbm[:5], cotangent_hbm, *weights_hbm[5:])
    loads = [
        pltpu.make_async_copy(src, dst, load_sem.at[t])
        for t, (src, dst) in enumerate(zip(sources, early + late))
    ]
    for load in loads:
        load.start()
    barrier = pltpu.get_barrier_semaphore()
    others = peers(row, col)
    for to_row, to_col, _ in others:
        pl.semaphore_signal(barrier, inc=1, device_id=(to_row, to_col), device_id_type=MESH)

    def start_all(phase, src, dst, same=False):
        for to_row, to_col, peer in others:
            pltpu.make_async_remote_copy(
                src_ref=src if same else src.at[peer],
                dst_ref=dst.at[me],
                send_sem=send_sem.at[phase],
                recv_sem=recv_sem.at[phase],
                device_id=(to_row, to_col),
                device_id_type=MESH,
            ).start()
        dst[me] = src[...] if same else src[me]

    def wait_on(sems, phase, dst):
        blocks_of = dst.at[pl.ds(0, n - 1)]
        pltpu.make_async_copy(blocks_of, blocks_of, sems.at[phase]).wait()

    def pack(dst, count, stride, first=0):
        def body(h, carry):
            at = pl.multiple_of(h * stride + first, 8)
            dst[h] = stage[pl.ds(at, count), :].astype(BF)
            return carry

        lax.fori_loop(0, n, body, 0, unroll=8)

    def unpack(src, count, stride, first=0):
        def body(h, carry):
            at = pl.multiple_of(h * stride + first, 8)
            stage[pl.ds(at, count), :] = src[h].astype(F32)
            return carry

        lax.fori_loop(0, n, body, 0, unroll=8)

    def spread(values, first, stride):
        for t in range(values.shape[1] // LANES):
            stage[pl.ds(first + t, LANES, stride=stride), :] = values[:, t * LANES : (t + 1) * LANES]

    def collect(first, stride, count):
        return jnp.concatenate(
            [stage[pl.ds(first + t, LANES, stride=stride), :] for t in range(count)], axis=1
        )

    def channels_first(ref, first):
        parts = []
        for t in range(GROUP):
            block = jnp.concatenate([ref[first + t], ref[first + t + half]], axis=0)
            parts.append(jnp.transpose(block.astype(F32)))
        return jnp.concatenate(parts, axis=1)

    def positions_first(ref, first, values):
        for t in range(GROUP):
            block = jnp.transpose(values[:, t * LANES : (t + 1) * LANES]).astype(BF)
            ref[first + t] = block[:cols]
            ref[first + t + half] = block[cols:]

    def lanes_at(first):
        return pl.ds(pl.multiple_of(first * LANES, LANES), wide)

    def assemble(src, at, count, dst):
        def body(r, carry):
            for q in range(n_col // 2):
                a = src[r * n_col + 2 * q, at : at + count, :].astype(F32)
                b = src[r * n_col + 2 * q + 1, at : at + count, :].astype(F32)
                both = jnp.concatenate(halves(a, b), axis=0).astype(BF)
                base = pl.multiple_of(r * 2 * count, 2 * count)
                dst[pl.ds(base, 2 * count), q * LANES : (q + 1) * LANES] = both
            return carry

        lax.fori_loop(0, n_row, body, 0, unroll=2)

    def disassemble(values, count, dst):
        for r in range(n_row):
            for q in range(n_col // 2):
                block = values[r * 2 * count : (r + 1) * 2 * count, q * LANES : (q + 1) * LANES]
                a, b = halves(block[:count], block[count:])
                dst[r * n_col + 2 * q] = a.astype(BF)
                dst[r * n_col + 2 * q + 1] = b.astype(BF)

    for load in loads[: len(early)]:
        load.wait()
    gain = column(norm_gain)
    bias = column(norm_bias)
    forward_weight = jnp.concatenate(
        [
            jnp.transpose(left_weight[...]),
            jnp.transpose(right_weight[...]),
            jnp.transpose(gate_weight[...]),
        ],
        axis=0,
    )

    def first_pass(g, carry):
        first = g * GROUP
        at = lanes_at(first)
        hat, scale = center_scale(channels_first(pair, first))
        normed = (hat * gain + bias).astype(BF)
        hat_s[:, at] = hat
        scale_s[:, at] = scale
        normed_s[:, at] = normed
        lane = lax.broadcasted_iota(jnp.int32, (1, wide), 1)
        inner = lax.rem(lane, LANES)
        i = row * rows + first + lane // LANES + inner // cols * half
        k = col * cols + lax.rem(inner, cols)
        real = length[0]
        mask = jnp.where((i < real) & (k < real), 1.0, 0.0).astype(F32)
        proj = dot(forward_weight, normed)
        for side in range(2):
            base = 2 * hidden * side
            sig = mask * jax.nn.sigmoid(proj[base + hidden : base + 2 * hidden])
            act = sig * proj[base : base + hidden]
            coef_s[2 * side, :, at] = sig
            coef_s[2 * side + 1, :, at] = act * (1.0 - sig)
            spread(act, first + (1 - side) * blocks, 40)
        gate_s[:, at] = jax.nn.sigmoid(proj[4 * hidden :])
        return carry

    lax.fori_loop(0, blocks // GROUP, first_pass, 0)
    pack(send_r, blocks, 40)
    for piece in range(2):
        pack(send_l.at[piece], part, 40, blocks + piece * part)
    pl.semaphore_wait(barrier, n - 1)
    start_all(0, send_r, recv_r)
    for piece in range(2):
        start_all(1 + piece, send_l.at[piece], recv_l.at[piece])

    for load in loads[len(early) :]:
        load.wait()
    o_gain = column(out_gain)
    o_bias = column(out_bias)
    out_back = out_weight[...]
    out_forward = jnp.transpose(out_back)
    zero = jnp.zeros((hidden, 1), F32)

    def early_pass(g, carry):
        first = g * GROUP
        at = lanes_at(first)
        upstream = channels_first(cotangent, first)
        up_s[:, at] = upstream.astype(BF)
        outer_grad = (upstream * gate_s[:, at]).astype(BF)
        ograd_s[:, at] = outer_grad
        tnorm_grad = dot(out_back, outer_grad)
        hgrad_s[:, at] = tnorm_grad
        return carry + jnp.sum(tnorm_grad, axis=1, keepdims=True)

    o_bias_grad = lax.fori_loop(0, blocks // GROUP, early_pass, zero)

    wait_on(recv_sem, 0, recv_r)
    assemble(recv_r, 0, blocks, big_r)
    for piece in range(2):
        wait_on(recv_sem, 1 + piece, recv_l.at[piece])
        assemble(recv_l.at[piece], 0, part, big_l.at[piece])
        disassemble(dot_last(big_l[piece], big_r[...]), part, send_b.at[piece])
        start_all(3 + piece, send_b.at[piece], recv_b.at[piece])

    for piece in range(2):
        wait_on(recv_sem, 3 + piece, recv_b.at[piece])
        unpack(recv_b.at[piece], part, 24)

        def second_pass(g, carry):
            first = g * GROUP
            at = lanes_at(piece * part + first)
            hat, scale = center_scale(collect(first, 24, GROUP))
            that_s[:, at] = hat
            spread(norm_back(hgrad_s[:, at] * o_gain, hat, scale), first, 24)
            return carry

        lax.fori_loop(0, groups, second_pass, 0)
        pack(send_c.at[piece], part, 24)
        start_all(5 + piece, send_c.at[piece], recv_c.at[piece])

    def late_pass(g, carry):
        first = g * GROUP
        at = lanes_at(first)
        hat = that_s[:, at]
        tri_normed = (hat * o_gain + o_bias).astype(BF)
        tnormed_s[:, at] = tri_normed
        gate = gate_s[:, at]
        gated = gate * dot(out_forward, tri_normed)
        positions_first(update, first, gated)
        ggrad_s[:, at] = (up_s[:, at].astype(F32) * gated * (1.0 - gate)).astype(BF)
        return carry + jnp.sum(hgrad_s[:, at] * hat, axis=1, keepdims=True)

    o_gain_grad = lax.fori_loop(0, blocks // GROUP, late_pass, zero)
    back_s[...] = dot(gate_weight[...], ggrad_s[...])
    part_output = dot_last(tnormed_s[...], ograd_s[...])
    part_gating = dot_last(normed_s[...], ggrad_s[...])

    for piece in range(2):
        wait_on(recv_sem, 5 + piece, recv_c.at[piece])
        here = pl.ds(piece * tokens // 2, tokens // 2)
        assemble(recv_c.at[piece], 0, part, big_g.at[here])
        disassemble(dot(big_g[here], big_r[...]), part, send_row.at[piece])
        start_all(7 + piece, send_row.at[piece], recv_row.at[piece])
    all_l = jnp.concatenate([big_l[0], big_l[1]], axis=0)
    col_own = dot_first(big_g[...], all_l)
    for r in range(n_row):
        for q in range(n_col // 2):
            block = col_own[r * rows : (r + 1) * rows, q * LANES : (q + 1) * LANES]
            for t, tile in enumerate(halves(block[:half], block[half:])):
                for piece in range(2):
                    send_col[piece, r * n_col + 2 * q + t] = tile[
                        piece * part : (piece + 1) * part
                    ].astype(BF)
    for piece in range(2):
        start_all(9 + piece, send_col.at[piece], recv_col.at[piece])

    def through(side, piece, phase, recv, weight):
        wait_on(recv_sem, phase + piece, recv.at[piece])
        unpack(recv.at[piece], part, 24)
        lines = slice(2 * hidden * side, 2 * hidden * (side + 1))

        def one(g, carry):
            first = g * GROUP
            at = lanes_at(piece * part + first)
            grad = collect(first, 24, GROUP)
            comb = jnp.concatenate(
                [grad * coef_s[2 * side, :, at], grad * coef_s[2 * side + 1, :, at]], axis=0
            ).astype(BF)
            comb_s[lines, at] = comb
            normed_grad = back_s[:, at] + dot(weight[...], comb)
            back_s[:, at] = normed_grad
            if side == 0:
                return carry
            along = normed_grad * hat_s[:, at]
            return (
                carry[0] + jnp.sum(along, axis=1, keepdims=True),
                carry[1] + jnp.sum(normed_grad, axis=1, keepdims=True),
            )

        sums = lax.fori_loop(0, groups, one, (zero, zero))
        held = slice(piece * part * LANES, (piece + 1) * part * LANES)
        return dot_last(normed_s[:, held], comb_s[lines, held]), sums

    lane = lax.broadcasted_iota(jnp.int32, (LANES, LANES), 1)

    def side_by_side(*columns):
        both = jnp.zeros((LANES, LANES), F32)
        for t, values in enumerate(columns):
            both = jnp.where(lane == t, values, both)
        return both

    def sum_up(recv):
        def add(p, total):
            return total + recv[p].astype(F32)

        zeros = jnp.zeros(recv.shape[1:], F32)
        return (lax.fori_loop(0, n, add, zeros, unroll=8) * (1.0 / tokens)).astype(BF)

    left_0, _ = through(0, 0, 7, recv_row, left_weight)
    left_1, _ = through(0, 1, 7, recv_row, left_weight)
    spread(left_0 + left_1, 0, 24)
    spread(part_gating, 2, 24)
    spread(part_output, 3, 24)
    pack(send_e, 4, 24)
    start_all(11, send_e, recv_e)
    right_0, sums_0 = through(1, 0, 9, recv_col, right_weight)
    right_1, sums_1 = through(1, 1, 9, recv_col, right_weight)
    spread(right_0 + right_1, 0, 24)
    gain_grad, bias_grad = sums_0[0] + sums_1[0], sums_0[1] + sums_1[1]
    spread(side_by_side(gain_grad, bias_grad, o_gain_grad, o_bias_grad), 2, 24)
    pack(send_h, 4, 24)
    start_all(12, send_h, recv_h)

    wait_on(recv_sem, 11, recv_e)
    send_f[...] = sum_up(recv_e)
    start_all(13, send_f, recv_f, same=True)

    def fourth_pass(g, carry):
        first = g * GROUP
        at = lanes_at(first)
        grad = norm_back(back_s[:, at] * gain, hat_s[:, at], scale_s[:, at])
        positions_first(grad_pair, first, grad)
        return carry

    lax.fori_loop(0, blocks // GROUP, fourth_pass, 0)

    wait_on(recv_sem, 12, recv_h)
    send_g[...] = sum_up(recv_h)
    start_all(14, send_g, recv_g, same=True)
    wait_on(recv_sem, 13, recv_f)
    unpack(recv_f, 4, 24)
    grad_left[...] = collect(0, 24, 2)
    grad_gating[...] = collect(2, 24, 1)
    grad_output[...] = collect(3, 24, 1)
    wait_on(recv_sem, 14, recv_g)
    unpack(recv_g, 4, 24)
    grad_right[...] = collect(0, 24, 2)
    grad_norms[...] = jnp.transpose(collect(2, 24, 1))[:4]
    halved = [
        dst.at[piece]
        for dst in (recv_l, recv_b, recv_c, recv_row, recv_col)
        for piece in range(2)
    ]
    for phase, dst in enumerate((recv_r, *halved, recv_e, recv_h, recv_f, recv_g)):
        wait_on(send_sem, phase, dst)


def finish(*refs):
    count = len(refs) // 2
    stores = [
        pltpu.make_async_copy(refs[t], refs[count + t], refs[-1].at[t]) for t in range(count)
    ]
    for store in stores:
        store.start()
    for store in stores:
        store.wait()


def per_device(pair, cotangent, length, *weights):
    n_row = lax.axis_size("row")
    n_col = lax.axis_size("col")
    n = n_row * n_col
    rows, cols, chan = pair.shape
    hidden = weights[-1].shape[0]
    tokens = n_row * rows
    places = rows * cols
    blocks = places // LANES
    part = blocks // 2
    weights = [w.reshape(1, -1) if w.ndim == 1 else w for w in weights]
    vmem = pl.BlockSpec(memory_space=pltpu.VMEM)
    shape = jax.ShapeDtypeStruct
    hbm = pl.BlockSpec(memory_space=pl.ANY)
    far = functools.partial(pltpu.with_memory_space_constraint, memory_space=pltpu.HBM)
    outs = (
        (pair.shape, BF),
        (pair.shape, BF),
        ((chan, 2 * hidden), F32),
        ((chan, 2 * hidden), F32),
        ((chan, chan), F32),
        ((hidden, chan), F32),
        ((4, chan), F32),
    )
    raw = pl.pallas_call(
        functools.partial(kernel, n_row, n_col),
        out_shape=tuple(pltpu.VMEM(*out) for out in outs),
        in_specs=[hbm, hbm, pl.BlockSpec(memory_space=pltpu.SMEM)] + [hbm] * len(weights),
        out_specs=(vmem,) * len(outs),
        scratch_shapes=[
            pltpu.VMEM(pair.shape, BF),
            *[pltpu.VMEM(w.shape, w.dtype) for w in weights[:5]],
            pltpu.VMEM(pair.shape, BF),
            *[pltpu.VMEM(w.shape, w.dtype) for w in weights[5:]],
            pltpu.VMEM((n * 40, LANES), F32),
            pltpu.VMEM((chan, places), F32),
            pltpu.VMEM((1, places), F32),
            pltpu.VMEM((chan, places), BF),
            pltpu.VMEM((4, hidden, places), F32),
            pltpu.VMEM((chan, places), F32),
            pltpu.VMEM((chan, places), BF),
            pltpu.VMEM((hidden, places), F32),
            pltpu.VMEM((hidden, places), F32),
            pltpu.VMEM((hidden, places), BF),
            pltpu.VMEM((chan, places), BF),
            pltpu.VMEM((chan, places), BF),
            pltpu.VMEM((chan, places), F32),
            pltpu.VMEM((4 * hidden, places), BF),
            pltpu.VMEM((2, tokens // 2, tokens), BF),
            pltpu.VMEM((tokens, tokens), BF),
            pltpu.VMEM((tokens, tokens), BF),
            *[pltpu.VMEM((n, blocks, LANES), BF)] * 2,
            *[pltpu.VMEM((2, n, part, LANES), BF)] * 10,
            *[pltpu.VMEM((n, 4, LANES), BF)] * 4,
            pltpu.VMEM((4, LANES), BF),
            pltpu.VMEM((n, 4, LANES), BF),
            pltpu.VMEM((4, LANES), BF),
            pltpu.VMEM((n, 4, LANES), BF),
            pltpu.SemaphoreType.DMA((15,)),
            pltpu.SemaphoreType.DMA((15,)),
            pltpu.SemaphoreType.DMA((10,)),
        ],
        compiler_params=pltpu.CompilerParams(
            collective_id=0, has_side_effects=True, vmem_limit_bytes=40 << 20
        ),
        name="triangle",
    )(far(pair), far(cotangent), length, *[far(w) for w in weights])
    raw = [pltpu.with_memory_space_constraint(a, pltpu.VMEM) for a in raw]
    return pl.pallas_call(
        finish,
        out_shape=tuple(shape(*out) for out in outs),
        in_specs=[vmem] * len(outs),
        out_specs=(hbm,) * len(outs),
        scratch_shapes=[pltpu.SemaphoreType.DMA((len(outs),))],
        compiler_params=pltpu.CompilerParams(vmem_limit_bytes=8 << 20),
        name="finish",
    )(*raw)


def solution(mesh):
    return jax.shard_map(
        per_device,
        mesh=mesh,
        in_specs=(P("row", "col", None), P("row", "col", None)) + (P(),) * 9,
        out_specs=(P("row", "col", None), P("row", "col", None)) + (P(),) * 5,
        check_vma=False,
    )
```

```python
import functools

import jax
import jax.numpy as jnp
from jax import lax
from jax.experimental import pallas as pl
from jax.experimental.pallas import tpu as pltpu
from jax.sharding import PartitionSpec as P

EPS = 1e-05
MESH = pl.DeviceIdType.MESH
BF = jnp.bfloat16
F32 = jnp.float32
LANES = 128
GROUP = 8


def dot(a, b):
    return jnp.dot(a, b, preferred_element_type=F32)


def dot_last(a, b):
    return lax.dot_general(a, b, (((1,), (1,)), ((), ())), preferred_element_type=F32)


def dot_first(a, b):
    return lax.dot_general(a, b, (((0,), (0,)), ((), ())), preferred_element_type=F32)


def center_scale(values):
    center = values - jnp.mean(values, axis=0, keepdims=True)
    inverse = lax.rsqrt(jnp.mean(center * center, axis=0, keepdims=True) + EPS)
    return center * inverse, inverse


def norm_back(grad, hat, scale):
    mean = jnp.mean(grad, axis=0, keepdims=True)
    along = jnp.mean(grad * hat, axis=0, keepdims=True)
    return scale * (grad - mean - hat * along)


def halves(a, b):
    half = a.shape[1] // 2
    first = lax.broadcasted_iota(jnp.int32, a.shape, 1) < half
    return (
        jnp.where(first, a, pltpu.roll(b, half, 1)),
        jnp.where(first, pltpu.roll(a, half, 1), b),
    )


def column(row_ref):
    return jnp.transpose(jnp.broadcast_to(row_ref[...], (LANES, LANES)))[:, :1]


def distance(step):
    return sum(min(d, 4 - d) for d in step[:3])


STEPS = [
    (dx, dy, dz, dc)
    for dx in range(4)
    for dy in range(4)
    for dz in range(4)
    for dc in range(2)
    if (dx, dy, dz, dc) != (0, 0, 0, 0)
]
STEPS.sort(key=lambda step: (-distance(step), step[3]))


def peers(row, col):
    z = row // 8 * 2 + lax.rem(col, 2)
    x = lax.rem(row // 2, 4)
    core = lax.rem(row, 2)
    y = col // 2
    at_x = [lax.rem(x + d, 4) * 2 for d in range(4)]
    at_y = [lax.rem(y + d, 4) * 2 for d in range(4)]
    at_z = [lax.rem(z + d, 4) for d in range(4)]
    high = [q // 2 * 8 for q in at_z]
    low = [lax.rem(q, 2) for q in at_z]
    at_core = [core, 1 - core]
    found = []
    for dx, dy, dz, dc in STEPS:
        to_row = high[dz] + at_x[dx] + at_core[dc]
        to_col = at_y[dy] + low[dz]
        found.append((to_row, to_col, to_row * 8 + to_col))
    return found


def kernel(
    n_row,
    n_col,
    pair_hbm,
    cotangent_hbm,
    length,
    *refs,
):
    weights_hbm, refs = refs[:8], refs[8:]
    kernel_body(n_row, n_col, pair_hbm, cotangent_hbm, length, weights_hbm, *refs)


def kernel_body(
    n_row,
    n_col,
    pair_hbm,
    cotangent_hbm,
    length,
    weights_hbm,
    update,
    grad_pair,
    grad_left,
    grad_right,
    grad_gating,
    grad_output,
    grad_norms,
    pair,
    norm_gain,
    norm_bias,
    left_weight,
    right_weight,
    gate_weight,
    cotangent,
    out_gain,
    out_bias,
    out_weight,
    stage,
    hat_s,
    scale_s,
    normed_s,
    coef_s,
    gate_s,
    up_s,
    hgrad_s,
    that_s,
    tnormed_s,
    ograd_s,
    ggrad_s,
    back_s,
    comb_s,
    big_l,
    big_r,
    big_g,
    send_r,
    recv_r,
    send_l,
    recv_l,
    send_b,
    recv_b,
    send_c,
    recv_c,
    send_row,
    recv_row,
    send_col,
    recv_col,
    send_e,
    recv_e,
    send_h,
    recv_h,
    send_f,
    recv_f,
    send_g,
    recv_g,
    send_sem,
    recv_sem,
    load_sem,
):
    n = n_row * n_col
    rows, cols, chan = pair.shape
    hidden = out_weight.shape[0]
    blocks = rows * cols // LANES
    tokens = n_row * rows
    half = rows // 2
    wide = GROUP * LANES
    part = blocks // 2
    groups = part // GROUP
    row = lax.axis_index("row")
    col = lax.axis_index("col")
    me = row * n_col + col

    early = (pair, norm_gain, norm_bias, left_weight, right_weight, gate_weight)
    late = (cotangent, out_gain, out_bias, out_weight)
    sources = (pair_hbm, *weights_hbm[:5], cotangent_hbm, *weights_hbm[5:])
    loads = [
        pltpu.make_async_copy(src, dst, load_sem.at[t])
        for t, (src, dst) in enumerate(zip(sources, early + late))
    ]
    for load in loads:
        load.start()
    barrier = pltpu.get_barrier_semaphore()
    others = peers(row, col)
    for to_row, to_col, _ in others:
        pl.semaphore_signal(barrier, inc=1, device_id=(to_row, to_col), device_id_type=MESH)

    def start_all(phase, src, dst, same=False):
        for to_row, to_col, peer in others:
            pltpu.make_async_remote_copy(
                src_ref=src if same else src.at[peer],
                dst_ref=dst.at[me],
                send_sem=send_sem.at[phase],
                recv_sem=recv_sem.at[phase],
                device_id=(to_row, to_col),
                device_id_type=MESH,
            ).start()
        dst[me] = src[...] if same else src[me]

    def wait_on(sems, phase, dst):
        blocks_of = dst.at[pl.ds(0, n - 1)]
        pltpu.make_async_copy(blocks_of, blocks_of, sems.at[phase]).wait()

    def pack(dst, count, stride, first=0):
        def body(h, carry):
            at = pl.multiple_of(h * stride + first, 8)
            dst[h] = stage[pl.ds(at, count), :].astype(BF)
            return carry

        lax.fori_loop(0, n, body, 0, unroll=16)

    def unpack(src, count, stride, first=0):
        def body(h, carry):
            at = pl.multiple_of(h * stride + first, 8)
            stage[pl.ds(at, count), :] = src[h].astype(F32)
            return carry

        lax.fori_loop(0, n, body, 0, unroll=16)

    def spread(values, first, stride):
        for t in range(values.shape[1] // LANES):
            stage[pl.ds(first + t, LANES, stride=stride), :] = values[:, t * LANES : (t + 1) * LANES]

    def collect(first, stride, count):
        return jnp.concatenate(
            [stage[pl.ds(first + t, LANES, stride=stride), :] for t in range(count)], axis=1
        )

    def channels_first(ref, first):
        parts = []
        for t in range(GROUP):
            block = jnp.concatenate([ref[first + t], ref[first + t + half]], axis=0)
            parts.append(jnp.transpose(block.astype(F32)))
        return jnp.concatenate(parts, axis=1)

    def positions_first(ref, first, values):
        for t in range(GROUP):
            block = jnp.transpose(values[:, t * LANES : (t + 1) * LANES]).astype(BF)
            ref[first + t] = block[:cols]
            ref[first + t + half] = block[cols:]

    def lanes_at(first):
        return pl.ds(pl.multiple_of(first * LANES, LANES), wide)

    def assemble(src, at, count, dst):
        def body(r, carry):
            for q in range(n_col // 2):
                a = src[r * n_col + 2 * q, at : at + count, :].astype(F32)
                b = src[r * n_col + 2 * q + 1, at : at + count, :].astype(F32)
                both = jnp.concatenate(halves(a, b), axis=0).astype(BF)
                base = pl.multiple_of(r * 2 * count, 2 * count)
                dst[pl.ds(base, 2 * count), q * LANES : (q + 1) * LANES] = both
            return carry

        lax.fori_loop(0, n_row, body, 0, unroll=4)

    def disassemble(values, count, dst):
        for r in range(n_row):
            for q in range(n_col // 2):
                block = values[r * 2 * count : (r + 1) * 2 * count, q * LANES : (q + 1) * LANES]
                a, b = halves(block[:count], block[count:])
                dst[r * n_col + 2 * q] = a.astype(BF)
                dst[r * n_col + 2 * q + 1] = b.astype(BF)

    for load in loads[: len(early)]:
        load.wait()
    gain = column(norm_gain)
    bias = column(norm_bias)
    forward_weight = jnp.concatenate(
        [
            jnp.transpose(left_weight[...]),
            jnp.transpose(right_weight[...]),
            jnp.transpose(gate_weight[...]),
        ],
        axis=0,
    )

    def first_pass(g, carry):
        first = g * GROUP
        at = lanes_at(first)
        hat, scale = center_scale(channels_first(pair, first))
        normed = (hat * gain + bias).astype(BF)
        hat_s[:, at] = hat
        scale_s[:, at] = scale
        normed_s[:, at] = normed
        lane = lax.broadcasted_iota(jnp.int32, (1, wide), 1)
        inner = lax.rem(lane, LANES)
        i = row * rows + first + lane // LANES + inner // cols * half
        k = col * cols + lax.rem(inner, cols)
        real = length[0]
        mask = jnp.where((i < real) & (k < real), 1.0, 0.0).astype(F32)
        proj = dot(forward_weight, normed)
        for side in range(2):
            base = 2 * hidden * side
            sig = mask * jax.nn.sigmoid(proj[base + hidden : base + 2 * hidden])
            act = sig * proj[base : base + hidden]
            coef_s[2 * side, :, at] = sig
            coef_s[2 * side + 1, :, at] = act * (1.0 - sig)
            spread(act, first + (1 - side) * blocks, 40)
        gate_s[:, at] = jax.nn.sigmoid(proj[4 * hidden :])
        return carry

    lax.fori_loop(0, blocks // GROUP, first_pass, 0)
    pack(send_r, blocks, 40)
    for piece in range(2):
        pack(send_l.at[piece], part, 40, blocks + piece * part)
    pl.semaphore_wait(barrier, n - 1)
    start_all(0, send_r, recv_r)
    for piece in range(2):
        start_all(1 + piece, send_l.at[piece], recv_l.at[piece])

    for load in loads[len(early) :]:
        load.wait()
    o_gain = column(out_gain)
    o_bias = column(out_bias)
    out_back = out_weight[...]
    out_forward = jnp.transpose(out_back)
    zero = jnp.zeros((hidden, 1), F32)

    def early_pass(g, carry):
        first = g * GROUP
        at = lanes_at(first)
        upstream = channels_first(cotangent, first)
        up_s[:, at] = upstream.astype(BF)
        outer_grad = (upstream * gate_s[:, at]).astype(BF)
        ograd_s[:, at] = outer_grad
        tnorm_grad = dot(out_back, outer_grad)
        hgrad_s[:, at] = tnorm_grad
        return carry + jnp.sum(tnorm_grad, axis=1, keepdims=True)

    o_bias_grad = lax.fori_loop(0, blocks // GROUP, early_pass, zero)

    wait_on(recv_sem, 0, recv_r)
    assemble(recv_r, 0, blocks, big_r)
    for piece in range(2):
        wait_on(recv_sem, 1 + piece, recv_l.at[piece])
        assemble(recv_l.at[piece], 0, part, big_l.at[piece])
        disassemble(dot_last(big_l[piece], big_r[...]), part, send_b.at[piece])
        start_all(3 + piece, send_b.at[piece], recv_b.at[piece])

    for piece in range(2):
        wait_on(recv_sem, 3 + piece, recv_b.at[piece])
        unpack(recv_b.at[piece], part, 24)

        def second_pass(g, carry):
            first = g * GROUP
            at = lanes_at(piece * part + first)
            hat, scale = center_scale(collect(first, 24, GROUP))
            that_s[:, at] = hat
            spread(norm_back(hgrad_s[:, at] * o_gain, hat, scale), first, 24)
            return carry

        lax.fori_loop(0, groups, second_pass, 0)
        pack(send_c.at[piece], part, 24)
        start_all(5 + piece, send_c.at[piece], recv_c.at[piece])

    def late_pass(g, carry):
        first = g * GROUP
        at = lanes_at(first)
        hat = that_s[:, at]
        tri_normed = (hat * o_gain + o_bias).astype(BF)
        tnormed_s[:, at] = tri_normed
        gate = gate_s[:, at]
        gated = gate * dot(out_forward, tri_normed)
        positions_first(update, first, gated)
        ggrad_s[:, at] = (up_s[:, at].astype(F32) * gated * (1.0 - gate)).astype(BF)
        return carry + jnp.sum(hgrad_s[:, at] * hat, axis=1, keepdims=True)

    o_gain_grad = lax.fori_loop(0, blocks // GROUP, late_pass, zero)
    back_s[...] = dot(gate_weight[...], ggrad_s[...])
    part_output = dot_last(tnormed_s[...], ograd_s[...])
    part_gating = dot_last(normed_s[...], ggrad_s[...])

    for piece in range(2):
        wait_on(recv_sem, 5 + piece, recv_c.at[piece])
        here = pl.ds(piece * tokens // 2, tokens // 2)
        assemble(recv_c.at[piece], 0, part, big_g.at[here])
        disassemble(dot(big_g[here], big_r[...]), part, send_row.at[piece])
        start_all(7 + piece, send_row.at[piece], recv_row.at[piece])
    all_l = jnp.concatenate([big_l[0], big_l[1]], axis=0)
    col_own = dot_first(big_g[...], all_l)
    for r in range(n_row):
        for q in range(n_col // 2):
            block = col_own[r * rows : (r + 1) * rows, q * LANES : (q + 1) * LANES]
            for t, tile in enumerate(halves(block[:half], block[half:])):
                for piece in range(2):
                    send_col[piece, r * n_col + 2 * q + t] = tile[
                        piece * part : (piece + 1) * part
                    ].astype(BF)
    for piece in range(2):
        start_all(9 + piece, send_col.at[piece], recv_col.at[piece])

    def through(side, piece, phase, recv, weight):
        wait_on(recv_sem, phase + piece, recv.at[piece])
        unpack(recv.at[piece], part, 24)
        lines = slice(2 * hidden * side, 2 * hidden * (side + 1))

        def one(g, carry):
            first = g * GROUP
            at = lanes_at(piece * part + first)
            grad = collect(first, 24, GROUP)
            comb = jnp.concatenate(
                [grad * coef_s[2 * side, :, at], grad * coef_s[2 * side + 1, :, at]], axis=0
            ).astype(BF)
            comb_s[lines, at] = comb
            normed_grad = back_s[:, at] + dot(weight[...], comb)
            back_s[:, at] = normed_grad
            if side == 0:
                return carry
            along = normed_grad * hat_s[:, at]
            return (
                carry[0] + jnp.sum(along, axis=1, keepdims=True),
                carry[1] + jnp.sum(normed_grad, axis=1, keepdims=True),
            )

        sums = lax.fori_loop(0, groups, one, (zero, zero))
        held = slice(piece * part * LANES, (piece + 1) * part * LANES)
        return dot_last(normed_s[:, held], comb_s[lines, held]), sums

    lane = lax.broadcasted_iota(jnp.int32, (LANES, LANES), 1)

    def side_by_side(*columns):
        both = jnp.zeros((LANES, LANES), F32)
        for t, values in enumerate(columns):
            both = jnp.where(lane == t, values, both)
        return both

    def sum_up(recv):
        def add(p, total):
            return total + recv[p].astype(F32)

        zeros = jnp.zeros(recv.shape[1:], F32)
        return (lax.fori_loop(0, n, add, zeros, unroll=32) * (1.0 / tokens)).astype(BF)

    left_0, _ = through(0, 0, 7, recv_row, left_weight)
    left_1, _ = through(0, 1, 7, recv_row, left_weight)
    spread(left_0 + left_1, 0, 24)
    spread(part_gating, 2, 24)
    spread(part_output, 3, 24)
    pack(send_e, 4, 24)
    start_all(11, send_e, recv_e)
    right_0, sums_0 = through(1, 0, 9, recv_col, right_weight)
    right_1, sums_1 = through(1, 1, 9, recv_col, right_weight)
    spread(right_0 + right_1, 0, 24)
    gain_grad, bias_grad = sums_0[0] + sums_1[0], sums_0[1] + sums_1[1]
    spread(side_by_side(gain_grad, bias_grad, o_gain_grad, o_bias_grad), 2, 24)
    pack(send_h, 4, 24)
    start_all(12, send_h, recv_h)

    wait_on(recv_sem, 11, recv_e)
    send_f[...] = sum_up(recv_e)
    start_all(13, send_f, recv_f, same=True)

    def fourth_pass(g, carry):
        first = g * GROUP
        at = lanes_at(first)
        grad = norm_back(back_s[:, at] * gain, hat_s[:, at], scale_s[:, at])
        positions_first(grad_pair, first, grad)
        return carry

    lax.fori_loop(0, blocks // GROUP, fourth_pass, 0)

    wait_on(recv_sem, 12, recv_h)
    send_g[...] = sum_up(recv_h)
    start_all(14, send_g, recv_g, same=True)
    wait_on(recv_sem, 13, recv_f)
    unpack(recv_f, 4, 24)
    grad_left[...] = collect(0, 24, 2)
    grad_gating[...] = collect(2, 24, 1)
    grad_output[...] = collect(3, 24, 1)
    wait_on(recv_sem, 14, recv_g)
    unpack(recv_g, 4, 24)
    grad_right[...] = collect(0, 24, 2)
    grad_norms[...] = jnp.transpose(collect(2, 24, 1))[:4]
    halved = [
        dst.at[piece]
        for dst in (recv_l, recv_b, recv_c, recv_row, recv_col)
        for piece in range(2)
    ]
    for phase, dst in enumerate((recv_r, *halved, recv_e, recv_h, recv_f, recv_g)):
        wait_on(send_sem, phase, dst)


def finish(*refs):
    count = len(refs) // 2
    stores = [
        pltpu.make_async_copy(refs[t], refs[count + t], refs[-1].at[t]) for t in range(count)
    ]
    for store in stores:
        store.start()
    for store in stores:
        store.wait()


def per_device(pair, cotangent, length, *weights):
    n_row = lax.axis_size("row")
    n_col = lax.axis_size("col")
    n = n_row * n_col
    rows, cols, chan = pair.shape
    hidden = weights[-1].shape[0]
    tokens = n_row * rows
    places = rows * cols
    blocks = places // LANES
    part = blocks // 2
    weights = [w.reshape(1, -1) if w.ndim == 1 else w for w in weights]
    vmem = pl.BlockSpec(memory_space=pltpu.VMEM)
    shape = jax.ShapeDtypeStruct
    hbm = pl.BlockSpec(memory_space=pl.ANY)
    far = functools.partial(pltpu.with_memory_space_constraint, memory_space=pltpu.HBM)
    outs = (
        (pair.shape, BF),
        (pair.shape, BF),
        ((chan, 2 * hidden), F32),
        ((chan, 2 * hidden), F32),
        ((chan, chan), F32),
        ((hidden, chan), F32),
        ((4, chan), F32),
    )
    raw = pl.pallas_call(
        functools.partial(kernel, n_row, n_col),
        out_shape=tuple(pltpu.VMEM(*out) for out in outs),
        in_specs=[hbm, hbm, pl.BlockSpec(memory_space=pltpu.SMEM)] + [hbm] * len(weights),
        out_specs=(vmem,) * len(outs),
        scratch_shapes=[
            pltpu.VMEM(pair.shape, BF),
            *[pltpu.VMEM(w.shape, w.dtype) for w in weights[:5]],
            pltpu.VMEM(pair.shape, BF),
            *[pltpu.VMEM(w.shape, w.dtype) for w in weights[5:]],
            pltpu.VMEM((n * 40 + 64, LANES), F32),
            pltpu.VMEM((chan, places), F32),
            pltpu.VMEM((1, places), F32),
            pltpu.VMEM((chan, places), BF),
            pltpu.VMEM((4, hidden, places), F32),
            pltpu.VMEM((chan, places), F32),
            pltpu.VMEM((chan, places), BF),
            pltpu.VMEM((hidden, places), F32),
            pltpu.VMEM((hidden, places), F32),
            pltpu.VMEM((hidden, places), BF),
            pltpu.VMEM((chan, places), BF),
            pltpu.VMEM((chan, places), BF),
            pltpu.VMEM((chan, places), F32),
            pltpu.VMEM((4 * hidden, places), BF),
            pltpu.VMEM((2, tokens // 2, tokens), BF),
            pltpu.VMEM((tokens, tokens), BF),
            pltpu.VMEM((tokens, tokens), BF),
            *[pltpu.VMEM((n, blocks, LANES), BF)] * 2,
            *[pltpu.VMEM((2, n, part, LANES), BF)] * 10,
            *[pltpu.VMEM((n, 4, LANES), BF)] * 4,
            pltpu.VMEM((4, LANES), BF),
            pltpu.VMEM((n, 4, LANES), BF),
            pltpu.VMEM((4, LANES), BF),
            pltpu.VMEM((n, 4, LANES), BF),
            pltpu.SemaphoreType.DMA((15,)),
            pltpu.SemaphoreType.DMA((15,)),
            pltpu.SemaphoreType.DMA((10,)),
        ],
        compiler_params=pltpu.CompilerParams(
            collective_id=0, has_side_effects=True, vmem_limit_bytes=40 << 20
        ),
        name="triangle",
    )(far(pair), far(cotangent), length, *[far(w) for w in weights])
    raw = [pltpu.with_memory_space_constraint(a, pltpu.VMEM) for a in raw]
    return pl.pallas_call(
        finish,
        out_shape=tuple(shape(*out) for out in outs),
        in_specs=[vmem] * len(outs),
        out_specs=(hbm,) * len(outs),
        scratch_shapes=[pltpu.SemaphoreType.DMA((len(outs),))],
        compiler_params=pltpu.CompilerParams(vmem_limit_bytes=8 << 20),
        name="finish",
    )(*raw)


def solution(mesh):
    return jax.shard_map(
        per_device,
        mesh=mesh,
        in_specs=(P("row", "col", None), P("row", "col", None)) + (P(),) * 9,
        out_specs=(P("row", "col", None), P("row", "col", None)) + (P(),) * 5,
        check_vma=False,
    )
```
